256 devices in a mesh: dp: 128 (over y, x, z), mp: 2 (over core).
Axes of the slice: x: 4, y: 4, z: 8, core: 2. Of those that a mesh axis runs over, the one named last changes fastest.
Arguments:
- media: bfloat16 [2048, 256, 1024], P('dp'), may hold values from -6 to 6
- slot_clip: int32 [2048], P('dp'), may hold values from 0 to 127, as said below
- time_table: bfloat16 [144, 1024], replicated, may hold values from -6 to 6
- latents_init: float32 [64, 1024], replicated, may hold values from -6 to 6
- media_gain: float32 [2, 1024], replicated, may hold values from 0.5 to 1.5
- latent_gain: float32 [2, 1024], replicated, may hold values from 0.5 to 1.5
- final_gain: float32 [1024], replicated, may hold values from 0.5 to 1.5
- w_query: bfloat16 [2, 1024, 512], P(None, None, 'mp'), may hold values from -24 to 24
- w_key: bfloat16 [2, 1024, 512], P(None, None, 'mp'), may hold values from -0.1875 to 0.1875
- w_value: bfloat16 [2, 1024, 512], P(None, None, 'mp'), may hold values from -0.1875 to 0.1875
- w_out: bfloat16 [2, 512, 1024], P(None, 'mp'), may hold values from -0.5 to 0.5
Outputs:
- resampled: float32 [128, 64, 1024], P('dp')
The draws below stay inside these ranges and needn't reach their ends.
Inputs may be any that keep to these rules, and one draw needn't show every extreme that they name: `slot_clip`: slot b lies on dp index b // 16, and its clip differs from that index by at most 4; differences of +4 and -4 both occur in every draw.
All inputs are finite; a program needn't handle non-finite values.
Results may differ from the reference program's by a relative error of at most 0.0085.
The reference program's roundings to bfloat16 on the way count: a program that leaves them out, or rounds other values in their place, can miss the bound.
Values may be sent and summed in bfloat16 or wider, within the bound.
A program may use at most 128 MiB of HBM per device.

```python
import math
import jax
import jax.numpy as jnp
from jax import lax

D = 1024
HEADS = 8
HEAD_DIM = 64
LATENTS = 64
PATCHES = 256
LAYERS = 2
FRAMES_DEV = 16
REACH = 4
INNER = 512
CLIPS = 128
BLOCKS = 2048
TIMES = 144
N_DP = 128


def draw_slot_clip(key, part):
    first, second, third, fourth = jax.random.split(jax.random.fold_in(key, 11), 4)
    pull = jax.random.randint(first, (CLIPS,), 1, 9)
    holder = jnp.arange(BLOCKS) // FRAMES_DEV
    shifts = jnp.arange(2 * REACH + 1) - REACH
    candidate = holder[:, None] + shifts[None, :]
    inside = (candidate >= 0) & (candidate < CLIPS)
    weights = jnp.where(inside, pull[jnp.clip(candidate, 0, CLIPS - 1)], 0)
    cumul = jnp.cumsum(weights, axis=1)
    ticket = jax.random.randint(second, (BLOCKS,), 0, 1048576) % cumul[:, -1]
    chosen = jnp.sum((cumul <= ticket[:, None]).astype(jnp.int32), axis=1)
    clip = jnp.take_along_axis(candidate, chosen[:, None], axis=1)[:, 0]
    upper = jax.random.randint(third, (), 0, CLIPS - REACH)
    lower = jax.random.randint(fourth, (), REACH, CLIPS)
    slots = jnp.arange(BLOCKS)
    clip = jnp.where(slots == upper * FRAMES_DEV, upper + REACH, clip)
    clip = jnp.where(slots == lower * FRAMES_DEV + FRAMES_DEV - 1, lower - REACH, clip)
    return clip.astype(jnp.int32)


def draw_w_query(key, part):
    base = jnp.clip(jax.random.normal(jax.random.fold_in(key, 5), (LAYERS, D, HEADS, HEAD_DIM), jnp.float32), -4.0, 4.0)
    scaled = base * 2.0 / math.sqrt(D)
    return scaled.reshape(LAYERS, D, HEADS * HEAD_DIM).astype(jnp.bfloat16)


def steps_of(key, shape, pieces, smallest, largest):
    loudness, own = 1.0, jax.random.fold_in(key, 6)
    for axis_at, parts in pieces:
        steps = jnp.exp(jax.random.uniform(jax.random.fold_in(own, axis_at), (parts,), jnp.float32, smallest / len(pieces), largest / len(pieces)))
        loudness = loudness * jnp.repeat(steps, shape[axis_at] // parts).reshape([-1 if axis == axis_at else 1 for axis in range(len(shape))])
    return loudness


def noise(own_key, shape, scale, reach, cuts=(), dtype=jnp.bfloat16):
    array = scale * jax.random.normal(own_key, shape, jnp.float32)
    if cuts:
        array = array * steps_of(own_key, shape, cuts, -0.22, 0.18)
    return jnp.clip(array, -reach, reach).astype(dtype)


def setup_inputs(seed: int = 0) -> dict:
    seeds = jax.random.split(jax.random.key(seed), 12)
    media = noise(seeds[0], (BLOCKS, PATCHES, D), 1.0, 6.0, ((0, 128),))
    slot_clip = draw_slot_clip(jax.random.fold_in(seeds[11], 71), 0)
    time_table = noise(seeds[2], (TIMES, D), 1.0, 6.0)
    latents_init = noise(seeds[3], (LATENTS, D), 1.0, 6.0, (), jnp.float32)
    media_gain = jnp.clip(1.0 + 0.1 * jax.random.normal(seeds[4], (LAYERS, D), jnp.float32), 0.5, 1.5)
    latent_gain = jnp.clip(1.0 + 0.1 * jax.random.normal(seeds[5], (LAYERS, D), jnp.float32), 0.5, 1.5)
    final_gain = jnp.clip(1.0 + 0.1 * jax.random.normal(seeds[6], (D,), jnp.float32), 0.5, 1.5)
    w_query = draw_w_query(jax.random.fold_in(seeds[11], 71), 0)
    w_key = noise(seeds[8], (LAYERS, D, INNER), D ** -0.5, 0.1875, ((2, 2),))
    w_value = noise(seeds[9], (LAYERS, D, INNER), D ** -0.5, 0.1875, ((2, 2),))
    w_out = noise(seeds[10], (LAYERS, INNER, D), (INNER // 4) ** -0.5, 0.5, ((1, 2),))
    return dict(media=media, slot_clip=slot_clip, time_table=time_table, latents_init=latents_init, media_gain=media_gain, latent_gain=latent_gain, final_gain=final_gain, w_query=w_query, w_key=w_key, w_value=w_value, w_out=w_out)


epsilon = 1e-05

def normalize(values):
    mean = lax.optimization_barrier(jnp.mean(values, axis=-1, keepdims=True))
    center = values - mean
    spread = lax.optimization_barrier(jnp.mean(center * center, axis=-1, keepdims=True))
    return center / jnp.sqrt(spread + epsilon)

def rounded(values):
    return lax.optimization_barrier(values.astype(jnp.bfloat16))

def block_stats(queries, keys, values):
    scores = jnp.einsum('qhd,khd->hqk', queries.astype(jnp.float32), keys.astype(jnp.float32))
    top = lax.optimization_barrier(jnp.max(scores, axis=-1))
    expo = jnp.exp(scores - top[..., None])
    total = lax.optimization_barrier(jnp.sum(expo, axis=-1))
    weights = rounded(expo).astype(jnp.float32)
    acc = jnp.einsum('hqk,khd->qhd', weights, values.astype(jnp.float32))
    return (top, total, acc)

def count_step(tally, clip):
    return (tally.at[clip].add(1), tally[clip])

def slot_stats(item):
    return block_stats(item[0], item[1], item[2])

def reference(media, slot_clip, time_table, latents_init, media_gain, latent_gain, final_gain, w_query, w_key, w_value, w_out):
    blocks, patches, width = media.shape
    clips = N_DP
    spent_tally, frame_index = lax.scan(count_step, jnp.zeros((clips,), jnp.int32), slot_clip)
    stamp = time_table[frame_index].astype(jnp.float32)
    unit = normalize(media.astype(jnp.float32) + stamp[:, None, :])
    state = jnp.broadcast_to(latents_init.astype(jnp.float32), (clips, LATENTS, width))
    for layer in range(LAYERS):
        lat_norm = rounded(normalize(state) * latent_gain[layer]).reshape(clips * LATENTS, width)
        query = rounded(jnp.dot(lat_norm, w_query[layer], preferred_element_type=jnp.float32) * HEAD_DIM ** (-0.5))
        query = query.reshape(clips, LATENTS, HEADS, HEAD_DIM)
        self_keys = rounded(jnp.dot(lat_norm, w_key[layer], preferred_element_type=jnp.float32)).reshape(clips, LATENTS, HEADS, HEAD_DIM)
        self_vals = rounded(jnp.dot(lat_norm, w_value[layer], preferred_element_type=jnp.float32)).reshape(clips, LATENTS, HEADS, HEAD_DIM)
        normed = rounded(unit * media_gain[layer]).reshape(blocks * patches, width)
        keys = rounded(jnp.dot(normed, w_key[layer], preferred_element_type=jnp.float32)).reshape(blocks, patches, HEADS, HEAD_DIM)
        vals = rounded(jnp.dot(normed, w_value[layer], preferred_element_type=jnp.float32)).reshape(blocks, patches, HEADS, HEAD_DIM)
        top, total, acc = lax.map(slot_stats, (query[slot_clip], keys, vals))
        own_top, own_total, own_acc = jax.vmap(block_stats)(query, self_keys, self_vals)
        best = own_top.at[slot_clip].max(top)
        weight = jnp.exp(top - best[slot_clip])
        own_weight = jnp.exp(own_top - best)
        whole = (own_weight * own_total).at[slot_clip].add(weight * total)
        combined = (own_acc * jnp.swapaxes(own_weight, 1, 2)[..., None]).at[slot_clip].add(acc * jnp.swapaxes(weight, 1, 2)[..., None])
        attn = rounded(combined / jnp.swapaxes(whole, 1, 2)[..., None]).reshape(clips * LATENTS, HEADS * HEAD_DIM)
        change = jnp.dot(attn, w_out[layer], preferred_element_type=jnp.float32)
        state = state + change.reshape(clips, LATENTS, width)
    return normalize(state) * final_gain
```

```python
import functools

import jax
import jax.numpy as jnp
from jax import lax
from jax.experimental import pallas as pl
from jax.experimental.pallas import tpu as pltpu
from jax.sharding import PartitionSpec as P

MESH = pl.DeviceIdType.MESH
HEAD_DIM = 64
LAYERS = 2
REACH = 4
SPAN = 2 * REACH + 1
BACK = 2 * REACH
EPS = 1e-05
FLOOR = -1e30
EARLY = 10
ORDER = (0, 8, 1, 7, 2, 6, 3, 5)

f32 = jnp.float32
bf16 = jnp.bfloat16


def normalize(values):
    mean = jnp.mean(values, axis=-1, keepdims=True)
    center = values - mean
    spread = jnp.mean(center * center, axis=-1, keepdims=True)
    return center * lax.rsqrt(spread + EPS)


def dot(a, b):
    return jnp.dot(a, b, preferred_element_type=f32)


def rows_to_lanes(tall, heads):
    rows = tall.shape[0] // heads
    return jnp.concatenate([tall[h * rows : (h + 1) * rows] for h in range(heads)], axis=1)


def kernel(
    n_dp,
    clip_s,
    clip_h,
    media_h,
    table_h,
    latents_h,
    mgain_h,
    lgain_h,
    fgain_h,
    wq_h,
    wk_h,
    wv_h,
    wo_h,
    out_ref,
    clip_v,
    near_clips,
    media,
    table,
    latents,
    mgain,
    lgain,
    fgain,
    wq,
    wkv,
    wo,
    stamps,
    norm_a,
    norm_b,
    norm1,
    k_a,
    k_b,
    v_a,
    v_b,
    k1,
    v1,
    accs,
    tops,
    totals,
    q_near,
    q_wide,
    part_acc,
    part_st,
    got_acc,
    got_st,
    attn_all,
    self_acc,
    self_st,
    state,
    local_sem,
    media_sem,
    clip_send,
    clip_recv,
    wo_send,
    wo_recv,
    acc_send,
    acc_recv,
    st_send,
    st_recv,
    q_send,
    q_recv,
    at_send,
    at_recv,
):
    frames, patches, width = media.shape
    inner = wq.shape[2]
    heads = inner // HEAD_DIM
    lat = latents.shape[0]
    hq = heads * lat
    me = lax.axis_index("dp")
    core = lax.axis_index("mp")

    def at(step):
        return (lax.rem(me + step + n_dp, n_dp), core)

    partner = (me, 1 - core)

    barrier = pltpu.get_barrier_semaphore()
    for step in range(1, BACK + 1):
        pl.semaphore_signal(barrier, inc=1, device_id=at(step), device_id_type=MESH)
        pl.semaphore_signal(barrier, inc=1, device_id=at(-step), device_id_type=MESH)
    pl.semaphore_signal(barrier, inc=1, device_id=partner, device_id_type=MESH)

    mine = pl.ds(pl.multiple_of(core * inner, inner), inner)
    loads = [
        (clip_h, clip_v),
        (latents_h, latents),
        (lgain_h, lgain),
        (mgain_h, mgain),
        (fgain_h, fgain),
        (wq_h, wq),
        (wk_h, wkv.at[:, :, pl.ds(0, inner)]),
        (wv_h, wkv.at[:, :, pl.ds(inner, inner)]),
        (table_h, table),
        (wo_h, wo.at[:, mine, :]),
    ]
    loads = [pltpu.make_async_copy(a, b, local_sem.at[i]) for i, (a, b) in enumerate(loads)]
    for copy in loads:
        copy.start()
    media_in = [pltpu.make_async_copy(media_h.at[f], media.at[f], media_sem.at[f]) for f in range(frames)]
    for copy in media_in:
        copy.start()

    loads[0].wait()
    pl.semaphore_wait(barrier, 2 * BACK + 1)
    clip_copies = [
        pltpu.make_async_remote_copy(
            src_ref=clip_v,
            dst_ref=near_clips.at[step - 1],
            send_sem=clip_send.at[step - 1],
            recv_sem=clip_recv.at[step - 1],
            device_id=at(step),
            device_id_type=MESH,
        )
        for step in range(1, BACK + 1)
    ]
    for copy in clip_copies[::-1]:
        copy.start()
    wo_copy = pltpu.make_async_remote_copy(
        src_ref=wo_h,
        dst_ref=wo.at[:, mine, :],
        send_sem=wo_send,
        recv_sem=wo_recv,
        device_id=partner,
        device_id_type=MESH,
    )
    wo_copy.start()

    row_head = lax.broadcasted_iota(jnp.int32, (inner, hq), 0) // HEAD_DIM
    lane_head = lax.broadcasted_iota(jnp.int32, (inner, hq), 1) // lat
    same_head = row_head == lane_head
    piece_head = lax.broadcasted_iota(jnp.int32, (HEAD_DIM, hq), 1) // lat

    def widen(compact):
        tiled = jnp.concatenate([compact] * heads, axis=0)
        return jnp.where(same_head, tiled, jnp.zeros_like(tiled))

    def block(keys, values, wide):
        scores = dot(keys, wide)
        top = jnp.max(scores, axis=0, keepdims=True)
        expo = jnp.exp(scores - top)
        total = jnp.sum(expo, axis=0, keepdims=True)
        full = lax.dot_general(
            values, expo.astype(bf16), (((0,), (0,)), ((), ())), preferred_element_type=f32
        )
        acc = full[0:HEAD_DIM]
        for h in range(1, heads):
            acc = jnp.where(piece_head == h, full[h * HEAD_DIM : (h + 1) * HEAD_DIM], acc)
        return top, total, acc

    def latent_side(layer):
        lat_norm = (normalize(state[...]) * lgain[layer : layer + 1, :]).astype(bf16)
        query = dot(lat_norm, wq[layer]) * (HEAD_DIM ** (-0.5))
        compact = rows_to_lanes(query.T, heads).astype(bf16)
        q_near[layer, REACH] = compact
        return lat_norm, compact

    def self_block(layer, lat_norm, compact):
        kv = dot(lat_norm, wkv[layer]).astype(bf16)
        top, total, acc = block(kv[:, :inner], kv[:, inner:], widen(compact))
        self_st[0:1, :] = top
        self_st[1:2, :] = total
        self_acc[...] = acc

    for copy in loads[1:9]:
        copy.wait()
    state[...] = latents[...]
    lat_norm, compact = latent_side(0)
    self_block(0, lat_norm, compact)
    q_wide[REACH] = widen(compact)

    row = lax.broadcasted_iota(jnp.int32, (frames, frames), 0)
    lane = lax.broadcasted_iota(jnp.int32, (frames, frames), 1)
    clip_col = jnp.zeros((frames, 1), jnp.int32)
    frame_row = lax.broadcasted_iota(jnp.int32, (frames, 1), 0)
    for f in range(frames):
        clip_col = jnp.where(frame_row == f, clip_s[f], clip_col)
    slot_col = clip_col - me + REACH
    own_row = clip_v[...]
    seen = jnp.where((clip_col == own_row) & (lane < row), 1.0, 0.0)
    for step in range(1, BACK + 1):
        clip_copies[step - 1].wait_recv()
        seen += jnp.where(clip_col == near_clips[step - 1], 1.0, 0.0)
    index = jnp.sum(seen, axis=1, keepdims=True).astype(jnp.int32)
    times = table.shape[0]
    picker = (lax.broadcasted_iota(jnp.int32, (frames, times), 1) == index).astype(f32).astype(bf16)
    stamps[...] = dot(picker, table[...])

    chunk = 16

    def norm_frame(f, dst):
        stamp = stamps[pl.ds(f, 1), :]
        for r in range(patches // chunk):
            rows = slice(r * chunk, (r + 1) * chunk)
            unit = normalize(media[f, rows, :].astype(f32) + stamp)
            dst[rows, :] = (unit * mgain[0:1, :]).astype(bf16)
            norm1[f, rows, :] = (unit * mgain[1:2, :]).astype(bf16)

    def project(src, k_dst, v_dst):
        kv = dot(src[...], wkv[0]).astype(bf16)
        k_dst[...] = kv[:, :inner]
        v_dst[...] = kv[:, inner:]

    def project1(f):
        kv = dot(norm1[f], wkv[1]).astype(bf16)
        k1[f] = kv[:, :inner]
        v1[f] = kv[:, inner:]

    def attend(f, keys, values, wide):
        top, total, acc = block(keys, values, wide)
        tops[pl.ds(f, 1), :] = top
        totals[pl.ds(f, 1), :] = total
        accs[f] = acc

    def media_wait(f):
        pltpu.make_async_copy(media_h.at[f], media.at[f], media_sem.at[f]).wait()

    wide0 = q_wide.at[REACH]
    media_wait(0)
    norm_frame(0, norm_a)
    media_wait(1)
    norm_frame(1, norm_b)
    project(norm_a, k_a, v_a)

    def pair(i, carry):
        f = 2 * i
        media_wait(f)
        media_wait(f + 1)
        norm_frame(f, norm_a)
        project(norm_b, k_b, v_b)
        attend(f - 2, k_a[...], v_a[...], wide0[...])
        norm_frame(f + 1, norm_b)
        project(norm_a, k_a, v_a)
        attend(f - 1, k_b[...], v_b[...], wide0[...])
        return carry

    lax.fori_loop(1, frames // 2, pair, 0)
    project(norm_b, k_b, v_b)
    attend(frames - 2, k_a[...], v_a[...], wide0[...])
    attend(frames - 1, k_b[...], v_b[...], wide0[...])

    def gather_part(layer, slot):
        chosen = slot_col == slot
        top = jnp.max(jnp.where(chosen, tops[...], FLOOR), axis=0, keepdims=True)
        weight = jnp.where(chosen, jnp.exp(jnp.where(chosen, tops[...] - top, 0.0)), 0.0)
        total = jnp.sum(weight * totals[...], axis=0, keepdims=True)
        acc = jnp.zeros((HEAD_DIM, hq), f32)
        for f in range(frames):
            acc += weight[f : f + 1, :] * accs[f]
        part_acc[layer, slot] = acc.astype(bf16)
        part_st[layer, slot, 0:1, :] = top
        part_st[layer, slot, 1:2, :] = total

    def part_copies(layer, slot):
        to = at(slot - REACH)
        return (
            pltpu.make_async_remote_copy(
                src_ref=part_st.at[layer, slot],
                dst_ref=got_st.at[layer, slot],
                send_sem=st_send.at[layer, slot],
                recv_sem=st_recv.at[layer, slot],
                device_id=to,
                device_id_type=MESH,
            ),
            pltpu.make_async_remote_copy(
                src_ref=part_acc.at[layer, slot],
                dst_ref=got_acc.at[layer, slot],
                send_sem=acc_send.at[layer, slot],
                recv_sem=acc_recv.at[layer, slot],
                device_id=to,
                device_id_type=MESH,
            ),
        )

    def send_parts(layer):
        for slot in ORDER:
            gather_part(layer, slot)
            for copy in part_copies(layer, slot):
                copy.start()
        gather_part(layer, REACH)

    def merge_parts(layer):
        for slot in ORDER:
            for copy in part_copies(layer, slot):
                copy.wait_recv()
        sources = [(self_st[0:1, :], self_st[1:2, :], self_acc)]
        sources.append((part_st[layer, REACH, 0:1, :], part_st[layer, REACH, 1:2, :], part_acc.at[layer, REACH]))
        for slot in ORDER:
            sources.append((got_st[layer, slot, 0:1, :], got_st[layer, slot, 1:2, :], got_acc.at[layer, slot]))
        best = functools.reduce(jnp.maximum, [top for top, _, _ in sources])
        whole = jnp.zeros_like(best)
        combined = jnp.zeros((HEAD_DIM, hq), f32)
        for top, total, acc in sources:
            weight = jnp.exp(top - best)
            whole += weight * total
            combined += weight * acc[...].astype(f32)
        return rows_to_lanes((combined / whole).T, heads).astype(bf16)

    def update_state(layer):
        attn_all[layer, :, mine] = merge_parts(layer)
        copy = pltpu.make_async_remote_copy(
            src_ref=attn_all.at[layer, :, mine],
            dst_ref=attn_all.at[layer, :, mine],
            send_sem=at_send.at[layer],
            recv_sem=at_recv.at[layer],
            device_id=partner,
            device_id_type=MESH,
        )
        copy.start()
        copy.wait_recv()
        state[...] += dot(attn_all[layer], wo[layer])
        return copy

    def loop1(start, stop):
        def step(f, carry):
            project1(f)
            return carry

        lax.fori_loop(start, stop, step, 0)

    send_parts(0)
    loop1(0, EARLY)
    loads[9].wait()
    wo_copy.wait()
    at0 = update_state(0)

    lat_norm, compact = latent_side(1)
    q_copies = [
        pltpu.make_async_remote_copy(
            src_ref=q_near.at[1, REACH],
            dst_ref=q_near.at[1, REACH - (slot - REACH)],
            send_sem=q_send.at[slot],
            recv_sem=q_recv.at[REACH - (slot - REACH)],
            device_id=at(slot - REACH),
            device_id_type=MESH,
        )
        for slot in ORDER
    ]
    for copy in q_copies:
        copy.start()
    self_block(1, lat_norm, compact)
    loop1(EARLY, frames)
    q_wide[REACH] = widen(compact)
    for slot, copy in zip(ORDER, q_copies):
        copy.wait_recv()
        q_wide[SPAN - 1 - slot] = widen(q_near[1, SPAN - 1 - slot])

    def attend1(i, carry):
        for f in (2 * i, 2 * i + 1):
            attend(f, k1[f], v1[f], q_wide[jnp.clip(clip_s[f] - me + REACH, 0, SPAN - 1)])
        return carry

    lax.fori_loop(0, frames // 2, attend1, 0)
    send_parts(1)
    at1 = update_state(1)
    out_ref[...] = normalize(state[...]) * fgain[...]

    for copy in clip_copies:
        copy.wait_send()
    for layer in range(LAYERS):
        for slot in ORDER:
            for copy in part_copies(layer, slot):
                copy.wait_send()
    for copy in q_copies:
        copy.wait_send()
    at0.wait_send()
    at1.wait_send()


def local(n_dp, media, slot_clip, table, latents, mgain, lgain, fgain, wq, wk, wv, wo):
    frames, patches, width = media.shape
    layers, _, inner = wq.shape
    heads = inner // HEAD_DIM
    lat = latents.shape[0]
    hq = heads * lat
    vmem, dma = pltpu.VMEM, pltpu.SemaphoreType.DMA
    scratch = [
        vmem((1, frames), jnp.int32),
        vmem((BACK, 1, frames), jnp.int32),
        vmem((frames, patches, width), bf16),
        vmem(table.shape, bf16),
        vmem(latents.shape, f32),
        vmem(mgain.shape, f32),
        vmem(lgain.shape, f32),
        vmem((1, width), f32),
        vmem(wq.shape, bf16),
        vmem((layers, width, 2 * inner), bf16),
        vmem((layers, 2 * inner, width), bf16),
        vmem((frames, width), f32),
        vmem((patches, width), bf16),
        vmem((patches, width), bf16),
        vmem((frames, patches, width), bf16),
        vmem((patches, inner), bf16),
        vmem((patches, inner), bf16),
        vmem((patches, inner), bf16),
        vmem((patches, inner), bf16),
        vmem((frames, patches, inner), bf16),
        vmem((frames, patches, inner), bf16),
        vmem((frames, HEAD_DIM, hq), f32),
        vmem((frames, hq), f32),
        vmem((frames, hq), f32),
        vmem((layers, SPAN, HEAD_DIM, hq), bf16),
        vmem((SPAN, inner, hq), bf16),
        vmem((layers, SPAN, HEAD_DIM, hq), bf16),
        vmem((layers, SPAN, 2, hq), f32),
        vmem((layers, SPAN, HEAD_DIM, hq), bf16),
        vmem((layers, SPAN, 2, hq), f32),
        vmem((layers, lat, 2 * inner), bf16),
        vmem((HEAD_DIM, hq), f32),
        vmem((2, hq), f32),
        vmem(latents.shape, f32),
        dma((10,)),
        dma((frames,)),
        dma((BACK,)),
        dma((BACK,)),
        dma(()),
        dma(()),
        dma((layers, SPAN)),
        dma((layers, SPAN)),
        dma((layers, SPAN)),
        dma((layers, SPAN)),
        dma((SPAN,)),
        dma((SPAN,)),
        dma((layers,)),
        dma((layers,)),
    ]
    result = pl.pallas_call(
        functools.partial(kernel, n_dp),
        out_shape=jax.ShapeDtypeStruct(latents.shape, f32),
        in_specs=[pl.BlockSpec(memory_space=pltpu.SMEM)] + [pl.BlockSpec(memory_space=pl.ANY)] * 11,
        out_specs=pl.BlockSpec(memory_space=pltpu.VMEM),
        scratch_shapes=scratch,
        compiler_params=pltpu.CompilerParams(
            collective_id=0, has_side_effects=True, vmem_limit_bytes=60 * 1024 * 1024
        ),
        name="resample",
    )(slot_clip, slot_clip[None, :], media, table, latents, mgain, lgain, fgain[None, :], wq, wk, wv, wo)
    return result[None]


def solution(mesh):
    return jax.shard_map(
        functools.partial(local, mesh.shape["dp"]),
        mesh=mesh,
        in_specs=(
            P("dp", None, None),
            P("dp"),
            P(),
            P(),
            P(),
            P(),
            P(),
            P(None, None, "mp"),
            P(None, None, "mp"),
            P(None, None, "mp"),
            P(None, "mp", None),
        ),
        out_specs=P("dp", None, None),
        check_vma=False,
    )
```

```python
import functools

import jax
import jax.numpy as jnp
from jax import lax
from jax.experimental import pallas as pl
from jax.experimental.pallas import tpu as pltpu
from jax.sharding import PartitionSpec as P

MESH = pl.DeviceIdType.MESH
HEAD_DIM = 64
LAYERS = 2
REACH = 4
SPAN = 2 * REACH + 1
BACK = 2 * REACH
EPS = 1e-05
FLOOR = -1e30
EARLY = 10
ORDER = (0, 8, 1, 7, 2, 6, 3, 5)

f32 = jnp.float32
bf16 = jnp.bfloat16


def normalize(values):
    mean = jnp.mean(values, axis=-1, keepdims=True)
    center = values - mean
    spread = jnp.mean(center * center, axis=-1, keepdims=True)
    return center * lax.rsqrt(spread + EPS)


def dot(a, b):
    return jnp.dot(a, b, preferred_element_type=f32)


def rows_to_lanes(tall, heads):
    rows = tall.shape[0] // heads
    return jnp.concatenate([tall[h * rows : (h + 1) * rows] for h in range(heads)], axis=1)


def kernel(
    n_dp,
    clip_s,
    clip_h,
    media_h,
    table_h,
    latents_h,
    mgain_h,
    lgain_h,
    fgain_h,
    wq_h,
    wk_h,
    wv_h,
    wo_h,
    out_ref,
    clip_v,
    near_clips,
    media,
    table,
    latents,
    mgain,
    lgain,
    fgain,
    wq,
    wkv,
    wo,
    stamps,
    norm_a,
    norm_b,
    scales,
    centered,
    k_a,
    k_b,
    v_a,
    v_b,
    k1,
    v1,
    accs,
    tops,
    totals,
    q_near,
    wide0,
    diagonal,
    part_acc,
    part_st,
    got_acc,
    got_st,
    attn_all,
    self_acc,
    self_st,
    state,
    local_sem,
    media_sem,
    clip_send,
    clip_recv,
    wo_send,
    wo_recv,
    acc_send,
    acc_recv,
    st_send,
    st_recv,
    q_send,
    q_recv,
    at_send,
    at_recv,
):
    frames, patches, width = media.shape
    inner = wq.shape[2]
    heads = inner // HEAD_DIM
    lat = latents.shape[0]
    hq = heads * lat
    me = lax.axis_index("dp")
    core = lax.axis_index("mp")

    def at(step):
        return (me + step, core)

    def near(step):
        return pl.when(me + step < n_dp if step > 0 else me + step >= 0)

    def beyond(step):
        return pl.when(me + step >= n_dp if step > 0 else me + step < 0)

    partner = (me, 1 - core)

    barrier = pltpu.get_barrier_semaphore()
    for step in (*range(-BACK, 0), *range(1, REACH + 1)):

        @near(step)
        def _():
            pl.semaphore_signal(barrier, inc=1, device_id=at(step), device_id_type=MESH)

    pl.semaphore_signal(barrier, inc=1, device_id=partner, device_id_type=MESH)

    mine = pl.ds(pl.multiple_of(core * inner, inner), inner)
    loads = [
        (clip_h, clip_v),
        (latents_h, latents),
        (lgain_h, lgain),
        (mgain_h, mgain),
        (fgain_h, fgain),
        (wq_h, wq),
        (wk_h, wkv.at[:, :, pl.ds(0, inner)]),
        (wv_h, wkv.at[:, :, pl.ds(inner, inner)]),
        (table_h, table),
        (wo_h, wo.at[:, mine, :]),
    ]
    loads = [pltpu.make_async_copy(a, b, local_sem.at[i]) for i, (a, b) in enumerate(loads)]
    for copy in loads:
        copy.start()
    media_in = [pltpu.make_async_copy(media_h.at[f], media.at[f], media_sem.at[f]) for f in range(frames)]
    for copy in media_in:
        copy.start()

    loads[0].wait()
    pl.semaphore_wait(barrier, jnp.minimum(BACK, n_dp - 1 - me) + jnp.minimum(REACH, me) + 1)
    clip_copies = [
        pltpu.make_async_remote_copy(
            src_ref=clip_v,
            dst_ref=near_clips.at[step - 1],
            send_sem=clip_send.at[step - 1],
            recv_sem=clip_recv.at[step - 1],
            device_id=at(step),
            device_id_type=MESH,
        )
        for step in range(1, BACK + 1)
    ]
    for step in range(BACK, 0, -1):
        near(step)(clip_copies[step - 1].start)
    wo_copy = pltpu.make_async_remote_copy(
        src_ref=wo_h,
        dst_ref=wo.at[:, mine, :],
        send_sem=wo_send,
        recv_sem=wo_recv,
        device_id=partner,
        device_id_type=MESH,
    )
    wo_copy.start()

    row_head = lax.broadcasted_iota(jnp.int32, (inner, hq), 0) // HEAD_DIM
    lane_head = lax.broadcasted_iota(jnp.int32, (inner, hq), 1) // lat
    diagonal[...] = (row_head == lane_head).astype(f32).astype(bf16)
    piece_head = lax.broadcasted_iota(jnp.int32, (HEAD_DIM, hq), 1) // lat

    def widen(compact):
        return jnp.concatenate([compact] * heads, axis=0) * diagonal[...]

    def block(keys, values, wide):
        scores = dot(keys, wide)
        top = jnp.max(scores, axis=0, keepdims=True)
        expo = jnp.exp(scores - top)
        total = jnp.sum(expo, axis=0, keepdims=True)
        full = lax.dot_general(
            values, expo.astype(bf16), (((0,), (0,)), ((), ())), preferred_element_type=f32
        )
        acc = full[0:HEAD_DIM]
        for h in range(1, heads):
            acc = jnp.where(piece_head == h, full[h * HEAD_DIM : (h + 1) * HEAD_DIM], acc)
        return top, total, acc

    def latent_side(layer):
        lat_norm = (normalize(state[...]) * lgain[layer : layer + 1, :]).astype(bf16)
        query = dot(lat_norm, wq[layer]) * (HEAD_DIM ** (-0.5))
        compact = rows_to_lanes(query.T, heads).astype(bf16)
        q_near[layer, REACH] = compact
        return lat_norm, compact

    def self_block(layer, lat_norm, compact):
        kv = dot(lat_norm, wkv[layer]).astype(bf16)
        top, total, acc = block(kv[:, :inner], kv[:, inner:], widen(compact))
        self_st[0:1, :] = top
        self_st[1:2, :] = total
        self_acc[...] = acc

    for step in range(1, BACK + 1):

        @beyond(-step)
        def _():
            near_clips[step - 1] = jnp.full(near_clips.shape[1:], -1, jnp.int32)

    for slot in ORDER:

        @beyond(REACH - slot)
        def _():
            for layer in range(LAYERS):
                got_st[layer, slot, 0:1, :] = jnp.full((1, hq), FLOOR, f32)
                got_st[layer, slot, 1:2, :] = jnp.zeros((1, hq), f32)
                got_acc[layer, slot] = jnp.zeros((HEAD_DIM, hq), bf16)

    for copy in loads[1:9]:
        copy.wait()
    state[...] = latents[...]
    lat_norm, compact = latent_side(0)
    self_block(0, lat_norm, compact)
    wide0[...] = widen(compact)

    chunk = 16

    def media_wait(f):
        pltpu.make_async_copy(media_h.at[f], media.at[f], media_sem.at[f]).wait()

    def center(f, carry):
        media_wait(f)
        for r in range(patches // chunk):
            rows = slice(r * chunk, (r + 1) * chunk)
            x = media[f, rows, :].astype(f32)
            centered[f, rows, :] = x - jnp.mean(x, axis=-1, keepdims=True)
        return carry

    lax.fori_loop(0, frames, center, 0)

    row = lax.broadcasted_iota(jnp.int32, (frames, frames), 0)
    lane = lax.broadcasted_iota(jnp.int32, (frames, frames), 1)
    clip_col = jnp.zeros((frames, 1), jnp.int32)
    frame_row = lax.broadcasted_iota(jnp.int32, (frames, 1), 0)
    for f in range(frames):
        clip_col = jnp.where(frame_row == f, clip_s[f], clip_col)
    slot_col = clip_col - me + REACH
    own_row = clip_v[...]
    seen = jnp.where((clip_col == own_row) & (lane < row), 1.0, 0.0)
    for step in range(1, BACK + 1):
        near(-step)(clip_copies[step - 1].wait_recv)
    for step in range(1, BACK + 1):
        seen += jnp.where(clip_col == near_clips[step - 1], 1.0, 0.0)
    index = jnp.sum(seen, axis=1, keepdims=True).astype(jnp.int32)
    times = table.shape[0]
    picker = (lax.broadcasted_iota(jnp.int32, (frames, times), 1) == index).astype(f32).astype(bf16)
    stamp = dot(picker, table[...])
    stamps[...] = stamp - jnp.mean(stamp, axis=-1, keepdims=True)

    def norm_frame(f, dst):
        stamp = stamps[pl.ds(f, 1), :]
        for r in range(patches // chunk):
            rows = slice(r * chunk, (r + 1) * chunk)
            value = centered[f, rows, :] + stamp
            scale = lax.rsqrt(jnp.mean(value * value, axis=-1, keepdims=True) + EPS)
            scales[f, rows, :] = jnp.broadcast_to(scale, (chunk, 128))
            dst[rows, :] = (value * scale * mgain[0:1, :]).astype(bf16)

    def norm_frame1(f, dst):
        stamp = stamps[pl.ds(f, 1), :]
        for r in range(patches // chunk):
            rows = slice(r * chunk, (r + 1) * chunk)
            value = centered[f, rows, :] + stamp
            scale = jnp.concatenate([scales[f, rows, :]] * (width // 128), axis=1)
            dst[rows, :] = (value * scale * mgain[1:2, :]).astype(bf16)

    def project(src, k_dst, v_dst):
        kv = dot(src[...], wkv[0]).astype(bf16)
        k_dst[...] = kv[:, :inner]
        v_dst[...] = kv[:, inner:]

    def project1(src, f):
        kv = dot(src[...], wkv[1]).astype(bf16)
        k1[f] = kv[:, :inner]
        v1[f] = kv[:, inner:]

    def attend(f, keys, values, wide):
        top, total, acc = block(keys, values, wide)
        tops[pl.ds(f, 1), :] = top
        totals[pl.ds(f, 1), :] = total
        accs[f] = acc

    norm_frame(0, norm_a)
    norm_frame(1, norm_b)
    project(norm_a, k_a, v_a)

    def pair(i, carry):
        f = 2 * i
        norm_frame(f, norm_a)
        project(norm_b, k_b, v_b)
        attend(f - 2, k_a[...], v_a[...], wide0[...])
        norm_frame(f + 1, norm_b)
        project(norm_a, k_a, v_a)
        attend(f - 1, k_b[...], v_b[...], wide0[...])
        return carry

    lax.fori_loop(1, frames // 2, pair, 0)
    project(norm_b, k_b, v_b)
    attend(frames - 2, k_a[...], v_a[...], wide0[...])
    attend(frames - 1, k_b[...], v_b[...], wide0[...])

    def gather_part(layer, slot):
        chosen = slot_col == slot
        top = jnp.max(jnp.where(chosen, tops[...], FLOOR), axis=0, keepdims=True)
        weight = jnp.where(chosen, jnp.exp(jnp.where(chosen, tops[...] - top, 0.0)), 0.0)
        total = jnp.sum(weight * totals[...], axis=0, keepdims=True)
        acc = jnp.zeros((HEAD_DIM, hq), f32)
        for f in range(frames):
            acc += weight[f : f + 1, :] * accs[f]
        part_acc[layer, slot] = acc.astype(bf16)
        part_st[layer, slot, 0:1, :] = top
        part_st[layer, slot, 1:2, :] = total

    def part_copies(layer, slot):
        to = at(slot - REACH)
        return (
            pltpu.make_async_remote_copy(
                src_ref=part_st.at[layer, slot],
                dst_ref=got_st.at[layer, slot],
                send_sem=st_send.at[layer, slot],
                recv_sem=st_recv.at[layer, slot],
                device_id=to,
                device_id_type=MESH,
            ),
            pltpu.make_async_remote_copy(
                src_ref=part_acc.at[layer, slot],
                dst_ref=got_acc.at[layer, slot],
                send_sem=acc_send.at[layer, slot],
                recv_sem=acc_recv.at[layer, slot],
                device_id=to,
                device_id_type=MESH,
            ),
        )

    def send_parts(layer):
        for slot in ORDER:
            gather_part(layer, slot)
            for copy in part_copies(layer, slot):
                near(slot - REACH)(copy.start)
        gather_part(layer, REACH)

    def merge_parts(layer):
        for slot in ORDER:
            for copy in part_copies(layer, slot):
                near(REACH - slot)(copy.wait_recv)
        sources = [(self_st[0:1, :], self_st[1:2, :], self_acc)]
        sources.append((part_st[layer, REACH, 0:1, :], part_st[layer, REACH, 1:2, :], part_acc.at[layer, REACH]))
        for slot in ORDER:
            sources.append((got_st[layer, slot, 0:1, :], got_st[layer, slot, 1:2, :], got_acc.at[layer, slot]))
        best = functools.reduce(jnp.maximum, [top for top, _, _ in sources])
        whole = jnp.zeros_like(best)
        combined = jnp.zeros((HEAD_DIM, hq), f32)
        for top, total, acc in sources:
            weight = jnp.exp(top - best)
            whole += weight * total
            combined += weight * acc[...].astype(f32)
        return rows_to_lanes((combined / whole).T, heads).astype(bf16)

    def update_state(layer):
        attn_all[layer, :, mine] = merge_parts(layer)
        copy = pltpu.make_async_remote_copy(
            src_ref=attn_all.at[layer, :, mine],
            dst_ref=attn_all.at[layer, :, mine],
            send_sem=at_send.at[layer],
            recv_sem=at_recv.at[layer],
            device_id=partner,
            device_id_type=MESH,
        )
        copy.start()
        copy.wait_recv()
        state[...] += dot(attn_all[layer], wo[layer])
        return copy

    def loop1(start, stop):
        def pair1(i, carry):
            f = 2 * i
            norm_frame1(f + 1, norm_b)
            project1(norm_a, f)
            norm_frame1(jnp.minimum(f + 2, frames - 1), norm_a)
            project1(norm_b, f + 1)
            return carry

        lax.fori_loop(start // 2, stop // 2, pair1, 0)

    send_parts(0)
    norm_frame1(0, norm_a)
    loop1(0, EARLY)
    loads[9].wait()
    wo_copy.wait()
    at0 = update_state(0)

    lat_norm, compact = latent_side(1)
    q_copies = [
        pltpu.make_async_remote_copy(
            src_ref=q_near.at[1, REACH],
            dst_ref=q_near.at[1, REACH - (slot - REACH)],
            send_sem=q_send.at[slot],
            recv_sem=q_recv.at[REACH - (slot - REACH)],
            device_id=at(slot - REACH),
            device_id_type=MESH,
        )
        for slot in ORDER
    ]
    for slot, copy in zip(ORDER, q_copies):
        near(slot - REACH)(copy.start)
    self_block(1, lat_norm, compact)
    loop1(EARLY, frames)
    for slot, copy in zip(ORDER, q_copies):
        near(REACH - slot)(copy.wait_recv)

    def attend1(i, carry):
        for j in range(4):
            f = 4 * i + j
            slot = jnp.clip(clip_s[f] - me + REACH, 0, SPAN - 1)
            attend(f, k1[f], v1[f], widen(q_near[1, slot]))
        return carry

    lax.fori_loop(0, frames // 4, attend1, 0)
    send_parts(1)
    at1 = update_state(1)
    out_ref[...] = normalize(state[...]) * fgain[...]

    for step in range(1, BACK + 1):
        near(step)(clip_copies[step - 1].wait_send)
    for slot, q_copy in zip(ORDER, q_copies):

        @near(slot - REACH)
        def _():
            q_copy.wait_send()
            for layer in range(LAYERS):
                for copy in part_copies(layer, slot):
                    copy.wait_send()

    at0.wait_send()
    at1.wait_send()


def local(n_dp, media, slot_clip, table, latents, mgain, lgain, fgain, wq, wk, wv, wo):
    frames, patches, width = media.shape
    layers, _, inner = wq.shape
    heads = inner // HEAD_DIM
    lat = latents.shape[0]
    hq = heads * lat
    vmem, dma = pltpu.VMEM, pltpu.SemaphoreType.DMA
    scratch = [
        vmem((1, frames), jnp.int32),
        vmem((BACK, 1, frames), jnp.int32),
        vmem((frames, patches, width), bf16),
        vmem(table.shape, bf16),
        vmem(latents.shape, f32),
        vmem(mgain.shape, f32),
        vmem(lgain.shape, f32),
        vmem((1, width), f32),
        vmem(wq.shape, bf16),
        vmem((layers, width, 2 * inner), bf16),
        vmem((layers, 2 * inner, width), bf16),
        vmem((frames, width), f32),
        vmem((patches, width), bf16),
        vmem((patches, width), bf16),
        vmem((frames, patches, 128), f32),
        vmem((frames, patches, width), f32),
        vmem((patches, inner), bf16),
        vmem((patches, inner), bf16),
        vmem((patches, inner), bf16),
        vmem((patches, inner), bf16),
        vmem((frames, patches, inner), bf16),
        vmem((frames, patches, inner), bf16),
        vmem((frames, HEAD_DIM, hq), f32),
        vmem((frames, hq), f32),
        vmem((frames, hq), f32),
        vmem((layers, SPAN, HEAD_DIM, hq), bf16),
        vmem((inner, hq), bf16),
        vmem((inner, hq), bf16),
        vmem((layers, SPAN, HEAD_DIM, hq), bf16),
        vmem((layers, SPAN, 2, hq), f32),
        vmem((layers, SPAN, HEAD_DIM, hq), bf16),
        vmem((layers, SPAN, 2, hq), f32),
        vmem((layers, lat, 2 * inner), bf16),
        vmem((HEAD_DIM, hq), f32),
        vmem((2, hq), f32),
        vmem(latents.shape, f32),
        dma((10,)),
        dma((frames,)),
        dma((BACK,)),
        dma((BACK,)),
        dma(()),
        dma(()),
        dma((layers, SPAN)),
        dma((layers, SPAN)),
        dma((layers, SPAN)),
        dma((layers, SPAN)),
        dma((SPAN,)),
        dma((SPAN,)),
        dma((layers,)),
        dma((layers,)),
    ]
    result = pl.pallas_call(
        functools.partial(kernel, n_dp),
        out_shape=jax.ShapeDtypeStruct(latents.shape, f32),
        in_specs=[pl.BlockSpec(memory_space=pltpu.SMEM)] + [pl.BlockSpec(memory_space=pl.ANY)] * 11,
        out_specs=pl.BlockSpec(memory_space=pltpu.VMEM),
        scratch_shapes=scratch,
        compiler_params=pltpu.CompilerParams(
            collective_id=0, has_side_effects=True, vmem_limit_bytes=60 * 1024 * 1024
        ),
        name="resample",
    )(slot_clip, slot_clip[None, :], media, table, latents, mgain, lgain, fgain[None, :], wq, wk, wv, wo)
    return result[None]


def solution(mesh):
    return jax.shard_map(
        functools.partial(local, mesh.shape["dp"]),
        mesh=mesh,
        in_specs=(
            P("dp", None, None),
            P("dp"),
            P(),
            P(),
            P(),
            P(),
            P(),
            P(None, None, "mp"),
            P(None, None, "mp"),
            P(None, None, "mp"),
            P(None, "mp", None),
        ),
        out_specs=P("dp", None, None),
        check_vma=False,
    )
```

```python
import functools

import jax
import jax.numpy as jnp
from jax import lax
from jax.experimental import pallas as pl
from jax.experimental.pallas import tpu as pltpu
from jax.sharding import PartitionSpec as P

MESH = pl.DeviceIdType.MESH
HEAD_DIM = 64
LAYERS = 2
REACH = 4
SPAN = 2 * REACH + 1
BACK = 2 * REACH
EPS = 1e-05
FLOOR = -1e30
GROUPS = 2
EARLY = 12
ORDER = (0, 8, 1, 7, 2, 6, 3, 5)

f32 = jnp.float32
bf16 = jnp.bfloat16


def normalize(values):
    mean = jnp.mean(values, axis=-1, keepdims=True)
    center = values - mean
    spread = jnp.mean(center * center, axis=-1, keepdims=True)
    return center * lax.rsqrt(spread + EPS)


def dot(a, b):
    return jnp.dot(a, b, preferred_element_type=f32)


def rows_to_lanes(tall, heads):
    rows = tall.shape[0] // heads
    return jnp.concatenate([tall[h * rows : (h + 1) * rows] for h in range(heads)], axis=1)


def other(slot):
    return slot - (slot > REACH)


def part(g, width):
    return slice(g * width, (g + 1) * width)


def kernel(
    n_dp,
    clip_s,
    clip_h,
    media_h,
    table_h,
    latents_h,
    mgain_h,
    lgain_h,
    fgain_h,
    wq_h,
    wk_h,
    wv_h,
    wo_h,
    out_ref,
    clip_v,
    near_clips,
    media,
    table,
    latents,
    mgain,
    lgain,
    fgain,
    wq,
    wkv,
    wo,
    stamps,
    norm_a,
    norm_b,
    scales,
    centered,
    kv_a,
    kv_b,
    kv0,
    p_a,
    p_b,
    kv1,
    accs,
    tops,
    totals,
    q_near_a,
    q_near_b,
    wide0,
    diagonal,
    part_acc,
    part_st,
    got_acc,
    got_st,
    attn_all,
    self_acc,
    self_st,
    state,
    local_sem,
    media_sem,
    clip_send,
    clip_recv,
    wo_send,
    wo_recv,
    acc_send,
    acc_recv,
    st_send,
    st_recv,
    q_send,
    q_recv,
    at_send,
    at_recv,
):
    frames, patches, width = media.shape
    inner = wq.shape[2]
    heads = inner // HEAD_DIM // GROUPS
    lat = latents.shape[0]
    hq = heads * lat
    hd = heads * HEAD_DIM
    me = lax.axis_index("dp")
    core = lax.axis_index("mp")

    def at(step):
        return (me + step, core)

    def near(step):
        return pl.when(me + step < n_dp if step > 0 else me + step >= 0)

    def beyond(step):
        return pl.when(me + step >= n_dp if step > 0 else me + step < 0)

    partner = (me, 1 - core)
    q_near = (q_near_a, q_near_b)

    barrier = pltpu.get_barrier_semaphore()
    for step in (*range(-BACK, 0), *range(1, REACH + 1)):

        @near(step)
        def _():
            pl.semaphore_signal(barrier, inc=1, device_id=at(step), device_id_type=MESH)

    pl.semaphore_signal(barrier, inc=1, device_id=partner, device_id_type=MESH)

    mine = pl.ds(pl.multiple_of(core * inner, inner), inner)
    step4 = 4

    def media_copy(i):
        rows = pl.ds(i * step4, step4)
        return pltpu.make_async_copy(media_h.at[rows], media.at[rows], media_sem.at[i])

    media_in = [media_copy(i) for i in range(frames // step4)]
    loads = [
        (clip_h, clip_v),
        (table_h, table),
        (latents_h, latents),
        (lgain_h, lgain),
        (mgain_h, mgain),
        (fgain_h, fgain),
        (wq_h, wq),
    ]
    for g in range(GROUPS):
        columns = pl.ds(g * hd, hd)
        loads.append((wk_h.at[:, :, columns], wkv.at[:, :, pl.ds(2 * g * hd, hd)]))
        loads.append((wv_h.at[:, :, columns], wkv.at[:, :, pl.ds((2 * g + 1) * hd, hd)]))
    loads.append((wo_h, wo.at[:, mine, :]))
    loads = [pltpu.make_async_copy(a, b, local_sem.at[i]) for i, (a, b) in enumerate(loads)]
    for copy in [loads[0]] + media_in + loads[1:]:
        copy.start()

    loads[0].wait()
    pl.semaphore_wait(barrier, jnp.minimum(BACK, n_dp - 1 - me) + jnp.minimum(REACH, me) + 1)
    clip_copies = [
        pltpu.make_async_remote_copy(
            src_ref=clip_v,
            dst_ref=near_clips.at[step - 1],
            send_sem=clip_send.at[step - 1],
            recv_sem=clip_recv.at[step - 1],
            device_id=at(step),
            device_id_type=MESH,
        )
        for step in range(1, BACK + 1)
    ]
    for step in range(BACK, 0, -1):
        near(step)(clip_copies[step - 1].start)
    wo_copy = pltpu.make_async_remote_copy(
        src_ref=wo_h,
        dst_ref=wo.at[:, mine, :],
        send_sem=wo_send,
        recv_sem=wo_recv,
        device_id=partner,
        device_id_type=MESH,
    )
    wo_copy.start()

    for step in range(1, BACK + 1):

        @beyond(-step)
        def _():
            near_clips[step - 1] = jnp.full(near_clips.shape[1:], -1, jnp.int32)

    for slot in ORDER:

        @beyond(REACH - slot)
        def _():
            for layer in range(LAYERS):
                for g in range(GROUPS):
                    got_st[layer, slot, 2 * g : 2 * g + 1, :] = jnp.full((1, hq), FLOOR, f32)
                    got_st[layer, slot, 2 * g + 1 : 2 * g + 2, :] = jnp.zeros((1, hq), f32)
                    got_acc[layer, g, slot] = jnp.zeros((HEAD_DIM, hq), bf16)

    chunk = 16

    def center(f, carry):
        for r in range(patches // chunk):
            x = media[f, part(r, chunk), :].astype(f32)
            centered[f, part(r, chunk), :] = x - jnp.mean(x, axis=-1, keepdims=True)
        return carry

    for i in range(frames // step4):
        media_in[i].wait()
        lax.fori_loop(i * step4, (i + 1) * step4, center, 0)

    row_head = lax.broadcasted_iota(jnp.int32, (hd, hq), 0) // HEAD_DIM
    lane_head = lax.broadcasted_iota(jnp.int32, (hd, hq), 1) // lat
    diagonal[...] = (row_head == lane_head).astype(f32).astype(bf16)
    piece_head = lax.broadcasted_iota(jnp.int32, (HEAD_DIM, hq), 1) // lat

    def widen(compact):
        return jnp.concatenate([compact] * heads, axis=0) * diagonal[...]

    def score(keys, wide):
        scores = dot(keys, wide)
        top = jnp.max(scores, axis=0, keepdims=True)
        expo = jnp.exp(scores - top)
        return top, jnp.sum(expo, axis=0, keepdims=True), expo.astype(bf16)

    def weigh(weights, values):
        full = lax.dot_general(values, weights, (((0,), (0,)), ((), ())), preferred_element_type=f32)
        acc = full[0:HEAD_DIM]
        for h in range(1, heads):
            acc = jnp.where(piece_head == h, full[part(h, HEAD_DIM)], acc)
        return acc

    def latent_side(layer):
        lat_norm = (normalize(state[...]) * lgain[layer : layer + 1, :]).astype(bf16)
        query = dot(lat_norm, wq[layer]) * (HEAD_DIM ** (-0.5))
        return lat_norm, [rows_to_lanes(query[:, part(g, hd)].T, heads).astype(bf16) for g in range(GROUPS)]

    def self_block(layer, lat_norm, compact):
        kv = dot(lat_norm, wkv[layer]).astype(bf16)
        for g in range(GROUPS):
            top, total, weights = score(kv[:, part(2 * g, hd)], widen(compact[g]))
            self_st[g, 0:1, :] = top
            self_st[g, 1:2, :] = total
            self_acc[g] = weigh(weights, kv[:, part(2 * g + 1, hd)])

    for copy in loads[1:-1]:
        copy.wait()
    state[...] = latents[...]
    lat_norm, compact = latent_side(0)
    self_block(0, lat_norm, compact)
    for g in range(GROUPS):
        wide0[g] = widen(compact[g])

    row = lax.broadcasted_iota(jnp.int32, (frames, frames), 0)
    lane = lax.broadcasted_iota(jnp.int32, (frames, frames), 1)
    clip_col = jnp.zeros((frames, 1), jnp.int32)
    frame_row = lax.broadcasted_iota(jnp.int32, (frames, 1), 0)
    for f in range(frames):
        clip_col = jnp.where(frame_row == f, clip_s[f], clip_col)
    slot_col = clip_col - me + REACH
    seen = jnp.where((clip_col == clip_v[...]) & (lane < row), 1.0, 0.0)
    for step in range(1, BACK + 1):
        near(-step)(clip_copies[step - 1].wait_recv)
    for step in range(1, BACK + 1):
        seen += jnp.where(clip_col == near_clips[step - 1], 1.0, 0.0)
    index = jnp.sum(seen, axis=1, keepdims=True).astype(jnp.int32)
    times = table.shape[0]
    picker = (lax.broadcasted_iota(jnp.int32, (frames, times), 1) == index).astype(f32).astype(bf16)
    stamp = dot(picker, table[...])
    stamps[...] = stamp - jnp.mean(stamp, axis=-1, keepdims=True)

    def norm_frame(f, dst):
        stamp = stamps[pl.ds(f, 1), :]
        for r in range(patches // chunk):
            rows = part(r, chunk)
            value = centered[f, rows, :] + stamp
            scale = lax.rsqrt(jnp.mean(value * value, axis=-1, keepdims=True) + EPS)
            scales[f, rows, :] = jnp.broadcast_to(scale, (chunk, 128))
            dst[rows, :] = (value * scale * mgain[0:1, :]).astype(bf16)

    def norm_frame1(f, dst):
        stamp = stamps[pl.ds(f, 1), :]
        for r in range(patches // chunk):
            rows = part(r, chunk)
            value = centered[f, rows, :] + stamp
            scale = jnp.concatenate([scales[f, rows, :]] * (width // 128), axis=1)
            dst[rows, :] = (value * scale * mgain[1:2, :]).astype(bf16)

    def project(f, src, dst):
        kv = dot(src[...], wkv[0]).astype(bf16)
        dst[...] = kv[:, : 2 * hd]
        kv0[f] = kv[:, 2 * hd :]

    def project1(src, f):
        kv1[f] = dot(src[...], wkv[1]).astype(bf16)

    def score_frame(g, f, keys, wide, dst):
        tops[g, pl.ds(f, 1), :], totals[g, pl.ds(f, 1), :], dst[...] = score(keys, wide)

    even, odd = (norm_a, kv_a, p_a), (norm_b, kv_b, p_b)

    def stage_norm(f, buffers):
        norm_frame(f, buffers[0])

    def stage_project(f, buffers):
        project(f, buffers[0], buffers[1])

    def stage_score(f, buffers):
        score_frame(0, f, buffers[1][:, :hd], wide0[0], buffers[2])

    def stage_weigh(f, buffers):
        accs[0, f] = weigh(buffers[2][...], buffers[1][:, hd:])

    stage_norm(0, even)
    stage_norm(1, odd)
    stage_project(0, even)
    stage_norm(2, even)
    stage_score(0, even)
    stage_project(1, odd)
    stage_norm(3, odd)
    stage_weigh(0, even)
    stage_score(1, odd)
    stage_project(2, even)

    def pair(i, carry):
        f = 2 * i
        stage_norm(f, even)
        stage_weigh(f - 3, odd)
        stage_score(f - 2, even)
        stage_project(f - 1, odd)
        stage_norm(f + 1, odd)
        stage_weigh(f - 2, even)
        stage_score(f - 1, odd)
        stage_project(f, even)
        return carry

    lax.fori_loop(2, frames // 2, pair, 0)
    stage_weigh(frames - 3, odd)
    stage_score(frames - 2, even)
    stage_project(frames - 1, odd)
    stage_weigh(frames - 2, even)
    stage_score(frames - 1, odd)
    stage_weigh(frames - 1, odd)

    def attend(score_at, weigh_at):
        def four(i, carry):
            f = 4 * i
            score_at(f + 1, p_b)
            weigh_at(f, p_a)
            score_at(f + 2, p_a)
            weigh_at(f + 1, p_b)
            score_at(f + 3, p_b)
            weigh_at(f + 2, p_a)
            score_at(jnp.minimum(f + 4, frames - 1), p_a)
            weigh_at(f + 3, p_b)
            return carry

        score_at(0, p_a)
        lax.fori_loop(0, frames // 4, four, 0)

    def score0(f, dst):
        score_frame(1, f, kv0[f, :, :hd], wide0[1], dst)

    def weigh0(f, src):
        accs[1, f] = weigh(src[...], kv0[f, :, hd:])

    def gather_part(layer, g, slot):
        chosen = slot_col == slot
        top = jnp.max(jnp.where(chosen, tops[g], FLOOR), axis=0, keepdims=True)
        weight = jnp.where(chosen, jnp.exp(jnp.where(chosen, tops[g] - top, 0.0)), 0.0)
        acc = jnp.zeros((HEAD_DIM, hq), f32)
        for f in range(frames):
            acc += weight[f : f + 1, :] * accs[g, f]
        part_acc[layer, g, slot] = acc.astype(bf16)
        part_st[layer, slot, 2 * g : 2 * g + 1, :] = top
        part_st[layer, slot, 2 * g + 1 : 2 * g + 2, :] = jnp.sum(weight * totals[g], axis=0, keepdims=True)

    def part_copies(layer, g, slot):
        copies = [
            pltpu.make_async_remote_copy(
                src_ref=part_acc.at[layer, g, slot],
                dst_ref=got_acc.at[layer, g, slot],
                send_sem=acc_send.at[g, other(slot)],
                recv_sem=acc_recv.at[g, other(slot)],
                device_id=at(slot - REACH),
                device_id_type=MESH,
            )
        ]
        if g == GROUPS - 1:
            copies.append(
                pltpu.make_async_remote_copy(
                    src_ref=part_st.at[layer, slot],
                    dst_ref=got_st.at[layer, slot],
                    send_sem=st_send.at[other(slot)],
                    recv_sem=st_recv.at[other(slot)],
                    device_id=at(slot - REACH),
                    device_id_type=MESH,
                )
            )
        return copies

    def send_parts(layer, g):
        for slot in ORDER:
            gather_part(layer, g, slot)
            copies = part_copies(layer, g, slot)

            @near(slot - REACH)
            def _():
                for copy in copies:
                    copy.start()

        gather_part(layer, g, REACH)

    def wait_parts(layer):
        for g in range(GROUPS):
            for slot in ORDER:
                copies = part_copies(layer, g, slot)

                @near(REACH - slot)
                def _():
                    for copy in copies:
                        copy.wait_recv()

    def wait_sent(layer):
        for slot in ORDER:

            @near(slot - REACH)
            def _():
                for g in range(GROUPS):
                    for copy in part_copies(layer, g, slot):
                        copy.wait_send()

    def merge_parts(layer, g):
        sources = [(self_st[g, 0:1, :], self_st[g, 1:2, :], self_acc.at[g])]
        for held_st, held_acc, slots in ((part_st, part_acc, (REACH,)), (got_st, got_acc, ORDER)):
            for slot in slots:
                held = (
                    held_st[layer, slot, 2 * g : 2 * g + 1, :],
                    held_st[layer, slot, 2 * g + 1 : 2 * g + 2, :],
                )
                sources.append((*held, held_acc.at[layer, g, slot]))
        best = functools.reduce(jnp.maximum, [top for top, _, _ in sources])
        whole = jnp.zeros_like(best)
        combined = jnp.zeros((HEAD_DIM, hq), f32)
        for top, total, acc in sources:
            weight = jnp.exp(top - best)
            whole += weight * total
            combined += weight * acc[...].astype(f32)
        return rows_to_lanes((combined / whole).T, heads).astype(bf16)

    def attn_copy(layer, g):
        columns = pl.ds(pl.multiple_of(core * inner + g * hd, hd), hd)
        return columns, pltpu.make_async_remote_copy(
            src_ref=attn_all.at[layer, :, columns],
            dst_ref=attn_all.at[layer, :, columns],
            send_sem=at_send.at[layer, g],
            recv_sem=at_recv.at[layer, g],
            device_id=partner,
            device_id_type=MESH,
        )

    def share_attn(layer, g):
        columns, copy = attn_copy(layer, g)
        attn_all[layer, :, columns] = merge_parts(layer, g)
        copy.start()

    def update_state(layer):
        for g in range(GROUPS):
            attn_copy(layer, g)[1].wait_recv()
        state[...] += dot(attn_all[layer], wo[layer])

    def loop1(start, stop):
        def pair1(i, carry):
            f = 2 * i
            norm_frame1(f + 1, norm_b)
            project1(norm_a, f)
            norm_frame1(jnp.minimum(f + 2, frames - 1), norm_a)
            project1(norm_b, f + 1)
            return carry

        lax.fori_loop(start // 2, stop // 2, pair1, 0)

    send_parts(0, 0)

    attend(score0, weigh0)
    send_parts(0, 1)

    norm_frame1(0, norm_a)
    loop1(0, EARLY)
    loads[-1].wait()
    wo_copy.wait()
    wait_parts(0)
    share_attn(0, 0)
    share_attn(0, 1)
    update_state(0)

    lat_norm, compact = latent_side(1)

    def q_copy(g, slot):
        return pltpu.make_async_remote_copy(
            src_ref=q_near[g].at[REACH],
            dst_ref=q_near[g].at[SPAN - 1 - slot],
            send_sem=q_send.at[g, other(slot)],
            recv_sem=q_recv.at[g, other(SPAN - 1 - slot)],
            device_id=at(slot - REACH),
            device_id_type=MESH,
        )

    for g in range(GROUPS):
        q_near[g][REACH] = compact[g]
    for g in range(GROUPS):
        for slot in ORDER:
            near(slot - REACH)(q_copy(g, slot).start)
    self_block(1, lat_norm, compact)
    loop1(EARLY, frames)
    wait_sent(0)

    def score1(g, f, dst):
        slot = jnp.clip(clip_s[f] - me + REACH, 0, SPAN - 1)
        score_frame(g, f, kv1[f, :, part(2 * g, hd)], widen(q_near[g][slot]), dst)

    def weigh1(g, f, src):
        accs[g, f] = weigh(src[...], kv1[f, :, part(2 * g + 1, hd)])

    for g in range(GROUPS):
        for slot in ORDER:
            near(REACH - slot)(q_copy(g, slot).wait_recv)

        attend(functools.partial(score1, g), functools.partial(weigh1, g))
        send_parts(1, g)

    wait_parts(1)
    share_attn(1, 0)
    share_attn(1, 1)
    update_state(1)
    out_ref[...] = normalize(state[...]) * fgain[...]

    for step in range(1, BACK + 1):
        near(step)(clip_copies[step - 1].wait_send)
    for slot in ORDER:

        @near(slot - REACH)
        def _():
            for g in range(GROUPS):
                q_copy(g, slot).wait_send()

    wait_sent(1)
    for layer in range(LAYERS):
        for g in range(GROUPS):
            attn_copy(layer, g)[1].wait_send()


def local(n_dp, media, slot_clip, table, latents, mgain, lgain, fgain, wq, wk, wv, wo):
    frames, patches, width = media.shape
    layers, _, inner = wq.shape
    heads = inner // HEAD_DIM // GROUPS
    lat = latents.shape[0]
    hq = heads * lat
    hd = heads * HEAD_DIM
    vmem, dma = pltpu.VMEM, pltpu.SemaphoreType.DMA
    scratch = [
        vmem((1, frames), jnp.int32),
        vmem((BACK, 1, frames), jnp.int32),
        vmem((frames, patches, width), bf16),
        vmem(table.shape, bf16),
        vmem(latents.shape, f32),
        vmem(mgain.shape, f32),
        vmem(lgain.shape, f32),
        vmem((1, width), f32),
        vmem(wq.shape, bf16),
        vmem((layers, width, 2 * inner), bf16),
        vmem((layers, 2 * inner, width), bf16),
        vmem((frames, width), f32),
        vmem((patches, width), bf16),
        vmem((patches, width), bf16),
        vmem((frames, patches, 128), f32),
        vmem((frames, patches, width), f32),
        vmem((patches, 2 * hd), bf16),
        vmem((patches, 2 * hd), bf16),
        vmem((frames, patches, 2 * hd), bf16),
        vmem((patches, hq), bf16),
        vmem((patches, hq), bf16),
        vmem((frames, patches, 2 * inner), bf16),
        vmem((GROUPS, frames, HEAD_DIM, hq), f32),
        vmem((GROUPS, frames, hq), f32),
        vmem((GROUPS, frames, hq), f32),
        vmem((SPAN, HEAD_DIM, hq), bf16),
        vmem((SPAN, HEAD_DIM, hq), bf16),
        vmem((GROUPS, hd, hq), bf16),
        vmem((hd, hq), bf16),
        vmem((layers, GROUPS, SPAN, HEAD_DIM, hq), bf16),
        vmem((layers, SPAN, 2 * GROUPS, hq), f32),
        vmem((layers, GROUPS, SPAN, HEAD_DIM, hq), bf16),
        vmem((layers, SPAN, 2 * GROUPS, hq), f32),
        vmem((layers, lat, 2 * inner), bf16),
        vmem((GROUPS, HEAD_DIM, hq), f32),
        vmem((GROUPS, 2, hq), f32),
        vmem(latents.shape, f32),
        dma((8 + 2 * GROUPS,)),
        dma((frames // 4,)),
        dma((BACK,)),
        dma((BACK,)),
        dma(()),
        dma(()),
        dma((GROUPS, BACK)),
        dma((GROUPS, BACK)),
        dma((BACK,)),
        dma((BACK,)),
        dma((GROUPS, BACK)),
        dma((GROUPS, BACK)),
        dma((layers, GROUPS)),
        dma((layers, GROUPS)),
    ]
    result = pl.pallas_call(
        functools.partial(kernel, n_dp),
        out_shape=pltpu.VMEM(latents.shape, f32),
        in_specs=[pl.BlockSpec(memory_space=pltpu.SMEM)] + [pl.BlockSpec(memory_space=pltpu.HBM)] * 11,
        out_specs=pl.BlockSpec(memory_space=pltpu.VMEM),
        scratch_shapes=scratch,
        compiler_params=pltpu.CompilerParams(
            collective_id=0, has_side_effects=True, vmem_limit_bytes=56 * 1024 * 1024
        ),
        name="resample",
    )(slot_clip, slot_clip[None, :], media, table, latents, mgain, lgain, fgain[None, :], wq, wk, wv, wo)
    return result[None]


def solution(mesh):
    return jax.shard_map(
        functools.partial(local, mesh.shape["dp"]),
        mesh=mesh,
        in_specs=(
            P("dp", None, None),
            P("dp"),
            P(),
            P(),
            P(),
            P(),
            P(),
            P(None, None, "mp"),
            P(None, None, "mp"),
            P(None, None, "mp"),
            P(None, "mp", None),
        ),
        out_specs=P("dp", None, None),
        check_vma=False,
    )
```

```python
import functools

import jax
import jax.numpy as jnp
from jax import lax
from jax.experimental import pallas as pl
from jax.experimental.pallas import tpu as pltpu
from jax.sharding import PartitionSpec as P

MESH = pl.DeviceIdType.MESH
HEAD_DIM = 64
LAYERS = 2
REACH = 4
SPAN = 2 * REACH + 1
BACK = 2 * REACH
EPS = 1e-05
FLOOR = -1e30
GROUPS = 2
STEP = 4
ATTEND = 16
AHEAD = 2
EARLY = 12
ORDER = (0, 8, 1, 7, 2, 6, 3, 5)

f32 = jnp.float32
bf16 = jnp.bfloat16


def normalize(values):
    mean = jnp.mean(values, axis=-1, keepdims=True)
    center = values - mean
    spread = jnp.mean(center * center, axis=-1, keepdims=True)
    return center * lax.rsqrt(spread + EPS)


def dot(a, b):
    return jnp.dot(a, b, preferred_element_type=f32)


def rows_to_lanes(tall, heads):
    rows = tall.shape[0] // heads
    return jnp.concatenate([tall[h * rows : (h + 1) * rows] for h in range(heads)], axis=1)


def other(slot):
    return slot - (slot > REACH)


def part(g, width):
    return slice(g * width, (g + 1) * width)


def kernel(
    n_dp,
    clip_s,
    clip_h,
    media_h,
    table_h,
    latents_h,
    mgain_h,
    lgain_h,
    fgain_h,
    wq_h,
    wk_h,
    wv_h,
    wo_h,
    out_ref,
    clip_v,
    near_clips,
    media,
    table,
    latents,
    mgain,
    lgain,
    fgain,
    wq,
    wkv,
    wo,
    stamps,
    norm_a,
    norm_b,
    scales,
    centered,
    kv0,
    p_a,
    p_b,
    p_c,
    p_d,
    kv1,
    accs,
    tops,
    totals,
    q_near_a,
    q_near_b,
    wide0,
    diagonal,
    part_acc,
    part_st,
    got_acc,
    got_st,
    attn_all,
    self_acc,
    self_st,
    state,
    local_sem,
    media_sem,
    clip_send,
    clip_recv,
    wo_send,
    wo_recv,
    acc_send,
    acc_recv,
    st_send,
    st_recv,
    q_send,
    q_recv,
    at_send,
    at_recv,
):
    frames, patches, width = media.shape
    inner = wq.shape[2]
    heads = inner // HEAD_DIM // GROUPS
    lat = latents.shape[0]
    hq = heads * lat
    hd = heads * HEAD_DIM
    me = lax.axis_index("dp")
    core = lax.axis_index("mp")

    def at(step):
        return (me + step, core)

    def near(step):
        return pl.when(me + step < n_dp if step > 0 else me + step >= 0)

    def beyond(step):
        return pl.when(me + step >= n_dp if step > 0 else me + step < 0)

    partner = (me, 1 - core)
    q_near = (q_near_a, q_near_b)

    barrier = pltpu.get_barrier_semaphore()
    for step in (*range(-BACK, 0), *range(1, REACH + 1)):

        @near(step)
        def _():
            pl.semaphore_signal(barrier, inc=1, device_id=at(step), device_id_type=MESH)

    pl.semaphore_signal(barrier, inc=1, device_id=partner, device_id_type=MESH)

    mine = pl.ds(pl.multiple_of(core * inner, inner), inner)
    step4 = 4

    def media_copy(i):
        rows = pl.ds(i * step4, step4)
        return pltpu.make_async_copy(media_h.at[rows], media.at[rows], media_sem.at[i])

    media_in = [media_copy(i) for i in range(frames // step4)]
    loads = [
        (clip_h, clip_v),
        (table_h, table),
        (latents_h, latents),
        (lgain_h, lgain),
        (mgain_h, mgain),
        (fgain_h, fgain),
        (wq_h, wq),
    ]
    for g in range(GROUPS):
        columns = pl.ds(g * hd, hd)
        loads.append((wk_h.at[:, :, columns], wkv.at[:, :, pl.ds(2 * g * hd, hd)]))
        loads.append((wv_h.at[:, :, columns], wkv.at[:, :, pl.ds((2 * g + 1) * hd, hd)]))
    loads.append((wo_h, wo.at[:, mine, :]))
    loads = [pltpu.make_async_copy(a, b, local_sem.at[i]) for i, (a, b) in enumerate(loads)]
    for copy in [loads[0]] + media_in + loads[1:]:
        copy.start()

    loads[0].wait()
    pl.semaphore_wait(barrier, jnp.minimum(BACK, n_dp - 1 - me) + jnp.minimum(REACH, me) + 1)
    clip_copies = [
        pltpu.make_async_remote_copy(
            src_ref=clip_v,
            dst_ref=near_clips.at[step - 1],
            send_sem=clip_send.at[step - 1],
            recv_sem=clip_recv.at[step - 1],
            device_id=at(step),
            device_id_type=MESH,
        )
        for step in range(1, BACK + 1)
    ]
    for step in range(BACK, 0, -1):
        near(step)(clip_copies[step - 1].start)
    wo_copy = pltpu.make_async_remote_copy(
        src_ref=wo_h,
        dst_ref=wo.at[:, mine, :],
        send_sem=wo_send,
        recv_sem=wo_recv,
        device_id=partner,
        device_id_type=MESH,
    )
    wo_copy.start()

    for step in range(1, BACK + 1):

        @beyond(-step)
        def _():
            near_clips[step - 1] = jnp.full(near_clips.shape[1:], -1, jnp.int32)

    for slot in ORDER:

        @beyond(REACH - slot)
        def _():
            for layer in range(LAYERS):
                for g in range(GROUPS):
                    got_st[layer, slot, 2 * g : 2 * g + 1, :] = jnp.full((1, hq), FLOOR, f32)
                    got_st[layer, slot, 2 * g + 1 : 2 * g + 2, :] = jnp.zeros((1, hq), f32)
                    got_acc[layer, g, slot] = jnp.zeros((HEAD_DIM, hq), bf16)

    chunk = 16

    def center(f, carry):
        for r in range(patches // chunk):
            x = media[f, part(r, chunk), :].astype(f32)
            centered[f, part(r, chunk), :] = x - jnp.mean(x, axis=-1, keepdims=True)
        return carry

    for i in range(frames // step4):
        media_in[i].wait()
        lax.fori_loop(i * step4, (i + 1) * step4, center, 0)

    row_head = lax.broadcasted_iota(jnp.int32, (hd, hq), 0) // HEAD_DIM
    lane_head = lax.broadcasted_iota(jnp.int32, (hd, hq), 1) // lat
    diagonal[...] = (row_head == lane_head).astype(f32).astype(bf16)
    piece_head = lax.broadcasted_iota(jnp.int32, (HEAD_DIM, hq), 1) // lat

    def widen(compact):
        return jnp.concatenate([compact] * heads, axis=0) * diagonal[...]

    def score(keys, wide):
        scores = dot(keys, wide)
        top = jnp.max(scores, axis=0, keepdims=True)
        expo = jnp.exp(scores - top)
        return top, jnp.sum(expo, axis=0, keepdims=True), expo.astype(bf16)

    def weigh(weights, values):
        full = lax.dot_general(values, weights, (((0,), (0,)), ((), ())), preferred_element_type=f32)
        acc = full[0:HEAD_DIM]
        for h in range(1, heads):
            acc = jnp.where(piece_head == h, full[part(h, HEAD_DIM)], acc)
        return acc

    def latent_side(layer):
        lat_norm = (normalize(state[...]) * lgain[layer : layer + 1, :]).astype(bf16)
        query = dot(lat_norm, wq[layer]) * (HEAD_DIM ** (-0.5))
        return lat_norm, [rows_to_lanes(query[:, part(g, hd)].T, heads).astype(bf16) for g in range(GROUPS)]

    def self_block(layer, lat_norm, compact):
        kv = dot(lat_norm, wkv[layer]).astype(bf16)
        for g in range(GROUPS):
            top, total, weights = score(kv[:, part(2 * g, hd)], widen(compact[g]))
            self_st[g, 0:1, :] = top
            self_st[g, 1:2, :] = total
            self_acc[g] = weigh(weights, kv[:, part(2 * g + 1, hd)])

    for copy in loads[1:-1]:
        copy.wait()
    state[...] = latents[...]
    lat_norm, compact = latent_side(0)
    self_block(0, lat_norm, compact)
    for g in range(GROUPS):
        wide0[g] = widen(compact[g])

    row = lax.broadcasted_iota(jnp.int32, (frames, frames), 0)
    lane = lax.broadcasted_iota(jnp.int32, (frames, frames), 1)
    clip_col = jnp.zeros((frames, 1), jnp.int32)
    frame_row = lax.broadcasted_iota(jnp.int32, (frames, 1), 0)
    for f in range(frames):
        clip_col = jnp.where(frame_row == f, clip_s[f], clip_col)
    slot_col = clip_col - me + REACH
    seen = jnp.where((clip_col == clip_v[...]) & (lane < row), 1.0, 0.0)
    for step in range(1, BACK + 1):
        near(-step)(clip_copies[step - 1].wait_recv)
    for step in range(1, BACK + 1):
        seen += jnp.where(clip_col == near_clips[step - 1], 1.0, 0.0)
    index = jnp.sum(seen, axis=1, keepdims=True).astype(jnp.int32)
    times = table.shape[0]
    picker = (lax.broadcasted_iota(jnp.int32, (frames, times), 1) == index).astype(f32).astype(bf16)
    stamp = dot(picker, table[...])
    stamps[...] = stamp - jnp.mean(stamp, axis=-1, keepdims=True)

    def norm_frame(f, dst):
        stamp = stamps[pl.ds(f, 1), :]
        for r in range(patches // chunk):
            rows = part(r, chunk)
            value = centered[f, rows, :] + stamp
            scale = lax.rsqrt(jnp.mean(value * value, axis=-1, keepdims=True) + EPS)
            scales[f, rows, :] = jnp.broadcast_to(scale, (chunk, 128))
            dst[rows, :] = (value * scale * mgain[0:1, :]).astype(bf16)

    def norm_frame1(f, dst):
        stamp = stamps[pl.ds(f, 1), :]
        for r in range(patches // chunk):
            rows = part(r, chunk)
            value = centered[f, rows, :] + stamp
            scale = jnp.concatenate([scales[f, rows, :]] * (width // 128), axis=1)
            dst[rows, :] = (value * scale * mgain[1:2, :]).astype(bf16)

    def project0(src, f):
        kv0[f] = dot(src[...], wkv[0]).astype(bf16)

    def project1(src, f):
        kv1[f] = dot(src[...], wkv[1]).astype(bf16)

    def score_frame(g, f, keys, wide, dst):
        tops[g, pl.ds(f, 1), :], totals[g, pl.ds(f, 1), :], dst[...] = score(keys, wide)

    p_all = (p_a, p_b, p_c, p_d)

    def norm_project(norm, project, start, stop, step):
        def several(i, carry):
            for j in range(step):
                f = step * i + j
                this, following = (norm_a, norm_b) if j % 2 == 0 else (norm_b, norm_a)
                norm(jnp.minimum(f + 1, frames - 1) if j == step - 1 else f + 1, following)
                project(this, f)
            return carry

        lax.fori_loop(start // step, stop // step, several, 0)

    norm_frame(0, norm_a)
    norm_project(norm_frame, project0, 0, frames, STEP)

    def attend(score_at, weigh_at):
        def several(i, carry):
            for j in range(ATTEND):
                f = ATTEND * i + j
                ahead = f + AHEAD
                score_at(jnp.minimum(ahead, frames - 1) if j + AHEAD >= ATTEND else ahead, p_all[(j + AHEAD) % len(p_all)])
                weigh_at(f, p_all[j % len(p_all)])
            return carry

        for j in range(AHEAD):
            score_at(j, p_all[j])
        lax.fori_loop(0, frames // ATTEND, several, 0)

    def score0(g, f, dst):
        score_frame(g, f, kv0[f, :, part(2 * g, hd)], wide0[g], dst)

    def weigh0(g, f, src):
        accs[g, f] = weigh(src[...], kv0[f, :, part(2 * g + 1, hd)])

    def gather_part(layer, g, slot):
        chosen = slot_col == slot
        top = jnp.max(jnp.where(chosen, tops[g], FLOOR), axis=0, keepdims=True)
        weight = jnp.where(chosen, jnp.exp(jnp.where(chosen, tops[g] - top, 0.0)), 0.0)
        acc = jnp.zeros((HEAD_DIM, hq), f32)
        for f in range(frames):
            acc += weight[f : f + 1, :] * accs[g, f]
        part_acc[layer, g, slot] = acc.astype(bf16)
        part_st[layer, slot, 2 * g : 2 * g + 1, :] = top
        part_st[layer, slot, 2 * g + 1 : 2 * g + 2, :] = jnp.sum(weight * totals[g], axis=0, keepdims=True)

    def part_copies(layer, g, slot):
        copies = [
            pltpu.make_async_remote_copy(
                src_ref=part_acc.at[layer, g, slot],
                dst_ref=got_acc.at[layer, g, slot],
                send_sem=acc_send.at[g, other(slot)],
                recv_sem=acc_recv.at[g, other(slot)],
                device_id=at(slot - REACH),
                device_id_type=MESH,
            )
        ]
        if g == GROUPS - 1:
            copies.append(
                pltpu.make_async_remote_copy(
                    src_ref=part_st.at[layer, slot],
                    dst_ref=got_st.at[layer, slot],
                    send_sem=st_send.at[other(slot)],
                    recv_sem=st_recv.at[other(slot)],
                    device_id=at(slot - REACH),
                    device_id_type=MESH,
                )
            )
        return copies

    def send_parts(layer, g):
        for slot in ORDER:
            gather_part(layer, g, slot)
            copies = part_copies(layer, g, slot)

            @near(slot - REACH)
            def _():
                for copy in copies:
                    copy.start()

        gather_part(layer, g, REACH)

    def wait_parts(layer):
        for g in range(GROUPS):
            for slot in ORDER:
                copies = part_copies(layer, g, slot)

                @near(REACH - slot)
                def _():
                    for copy in copies:
                        copy.wait_recv()

    def wait_sent(layer):
        for slot in ORDER:

            @near(slot - REACH)
            def _():
                for g in range(GROUPS):
                    for copy in part_copies(layer, g, slot):
                        copy.wait_send()

    def merge_parts(layer, g):
        sources = [(self_st[g, 0:1, :], self_st[g, 1:2, :], self_acc.at[g])]
        for held_st, held_acc, slots in ((part_st, part_acc, (REACH,)), (got_st, got_acc, ORDER)):
            for slot in slots:
                held = (
                    held_st[layer, slot, 2 * g : 2 * g + 1, :],
                    held_st[layer, slot, 2 * g + 1 : 2 * g + 2, :],
                )
                sources.append((*held, held_acc.at[layer, g, slot]))
        best = functools.reduce(jnp.maximum, [top for top, _, _ in sources])
        whole = jnp.zeros_like(best)
        combined = jnp.zeros((HEAD_DIM, hq), f32)
        for top, total, acc in sources:
            weight = jnp.exp(top - best)
            whole += weight * total
            combined += weight * acc[...].astype(f32)
        return rows_to_lanes((combined / whole).T, heads).astype(bf16)

    def attn_copy(layer, g):
        columns = pl.ds(pl.multiple_of(core * inner + g * hd, hd), hd)
        return columns, pltpu.make_async_remote_copy(
            src_ref=attn_all.at[layer, :, columns],
            dst_ref=attn_all.at[layer, :, columns],
            send_sem=at_send.at[layer, g],
            recv_sem=at_recv.at[layer, g],
            device_id=partner,
            device_id_type=MESH,
        )

    def share_attn(layer, g):
        columns, copy = attn_copy(layer, g)
        attn_all[layer, :, columns] = merge_parts(layer, g)
        copy.start()

    def update_state(layer):
        theirs = pl.ds(pl.multiple_of((1 - core) * inner, inner), inner)
        state[...] += dot(attn_all[layer, :, mine], wo[layer, mine, :])
        for g in range(GROUPS):
            attn_copy(layer, g)[1].wait_recv()
        state[...] += dot(attn_all[layer, :, theirs], wo[layer, theirs, :])

    for g in range(GROUPS):
        attend(functools.partial(score0, g), functools.partial(weigh0, g))
        send_parts(0, g)

    norm_frame1(0, norm_a)
    norm_project(norm_frame1, project1, 0, EARLY, 2)
    loads[-1].wait()
    wo_copy.wait()
    wait_parts(0)
    share_attn(0, 0)
    share_attn(0, 1)
    update_state(0)

    lat_norm, compact = latent_side(1)

    def q_copy(g, slot):
        return pltpu.make_async_remote_copy(
            src_ref=q_near[g].at[REACH],
            dst_ref=q_near[g].at[SPAN - 1 - slot],
            send_sem=q_send.at[g, other(slot)],
            recv_sem=q_recv.at[g, other(SPAN - 1 - slot)],
            device_id=at(slot - REACH),
            device_id_type=MESH,
        )

    for g in range(GROUPS):
        q_near[g][REACH] = compact[g]
    for g in range(GROUPS):
        for slot in ORDER:
            near(slot - REACH)(q_copy(g, slot).start)
    self_block(1, lat_norm, compact)
    norm_project(norm_frame1, project1, EARLY, frames, 2)
    wait_sent(0)

    def score1(g, f, dst):
        slot = jnp.clip(clip_s[f] - me + REACH, 0, SPAN - 1)
        score_frame(g, f, kv1[f, :, part(2 * g, hd)], widen(q_near[g][slot]), dst)

    def weigh1(g, f, src):
        accs[g, f] = weigh(src[...], kv1[f, :, part(2 * g + 1, hd)])

    for g in range(GROUPS):
        for slot in ORDER:
            near(REACH - slot)(q_copy(g, slot).wait_recv)

        attend(functools.partial(score1, g), functools.partial(weigh1, g))
        send_parts(1, g)

    wait_parts(1)
    share_attn(1, 0)
    share_attn(1, 1)
    update_state(1)
    out_ref[...] = normalize(state[...]) * fgain[...]

    for step in range(1, BACK + 1):
        near(step)(clip_copies[step - 1].wait_send)
    for slot in ORDER:

        @near(slot - REACH)
        def _():
            for g in range(GROUPS):
                q_copy(g, slot).wait_send()

    wait_sent(1)
    for layer in range(LAYERS):
        for g in range(GROUPS):
            attn_copy(layer, g)[1].wait_send()


def local(n_dp, media, slot_clip, table, latents, mgain, lgain, fgain, wq, wk, wv, wo):
    frames, patches, width = media.shape
    layers, _, inner = wq.shape
    heads = inner // HEAD_DIM // GROUPS
    lat = latents.shape[0]
    hq = heads * lat
    hd = heads * HEAD_DIM
    vmem, dma = pltpu.VMEM, pltpu.SemaphoreType.DMA
    scratch = [
        vmem((1, frames), jnp.int32),
        vmem((BACK, 1, frames), jnp.int32),
        vmem((frames, patches, width), bf16),
        vmem(table.shape, bf16),
        vmem(latents.shape, f32),
        vmem(mgain.shape, f32),
        vmem(lgain.shape, f32),
        vmem((1, width), f32),
        vmem(wq.shape, bf16),
        vmem((layers, width, 2 * inner), bf16),
        vmem((layers, 2 * inner, width), bf16),
        vmem((frames, width), f32),
        vmem((patches, width), bf16),
        vmem((patches, width), bf16),
        vmem((frames, patches, 128), f32),
        vmem((frames, patches, width), f32),
        vmem((frames, patches, 2 * inner), bf16),
        vmem((patches, hq), bf16),
        vmem((patches, hq), bf16),
        vmem((patches, hq), bf16),
        vmem((patches, hq), bf16),
        vmem((frames, patches, 2 * inner), bf16),
        vmem((GROUPS, frames, HEAD_DIM, hq), f32),
        vmem((GROUPS, frames, hq), f32),
        vmem((GROUPS, frames, hq), f32),
        vmem((SPAN, HEAD_DIM, hq), bf16),
        vmem((SPAN, HEAD_DIM, hq), bf16),
        vmem((GROUPS, hd, hq), bf16),
        vmem((hd, hq), bf16),
        vmem((layers, GROUPS, SPAN, HEAD_DIM, hq), bf16),
        vmem((layers, SPAN, 2 * GROUPS, hq), f32),
        vmem((layers, GROUPS, SPAN, HEAD_DIM, hq), bf16),
        vmem((layers, SPAN, 2 * GROUPS, hq), f32),
        vmem((layers, lat, 2 * inner), bf16),
        vmem((GROUPS, HEAD_DIM, hq), f32),
        vmem((GROUPS, 2, hq), f32),
        vmem(latents.shape, f32),
        dma((8 + 2 * GROUPS,)),
        dma((frames // 4,)),
        dma((BACK,)),
        dma((BACK,)),
        dma(()),
        dma(()),
        dma((GROUPS, BACK)),
        dma((GROUPS, BACK)),
        dma((BACK,)),
        dma((BACK,)),
        dma((GROUPS, BACK)),
        dma((GROUPS, BACK)),
        dma((layers, GROUPS)),
        dma((layers, GROUPS)),
    ]
    result = pl.pallas_call(
        functools.partial(kernel, n_dp),
        out_shape=pltpu.VMEM(latents.shape, f32),
        in_specs=[pl.BlockSpec(memory_space=pltpu.SMEM)] + [pl.BlockSpec(memory_space=pltpu.HBM)] * 11,
        out_specs=pl.BlockSpec(memory_space=pltpu.VMEM),
        scratch_shapes=scratch,
        compiler_params=pltpu.CompilerParams(
            collective_id=0, has_side_effects=True, vmem_limit_bytes=56 * 1024 * 1024
        ),
        name="resample",
    )(slot_clip, slot_clip[None, :], media, table, latents, mgain, lgain, fgain[None, :], wq, wk, wv, wo)
    return result[None]


def solution(mesh):
    return jax.shard_map(
        functools.partial(local, mesh.shape["dp"]),
        mesh=mesh,
        in_specs=(
            P("dp", None, None),
            P("dp"),
            P(),
            P(),
            P(),
            P(),
            P(),
            P(None, None, "mp"),
            P(None, None, "mp"),
            P(None, None, "mp"),
            P(None, "mp", None),
        ),
        out_specs=P("dp", None, None),
        check_vma=False,
    )
```

```python
import functools

import jax
import jax.numpy as jnp
from jax import lax
from jax.experimental import pallas as pl
from jax.experimental.pallas import tpu as pltpu
from jax.sharding import PartitionSpec as P

MESH = pl.DeviceIdType.MESH
HEAD_DIM = 64
LAYERS = 2
REACH = 4
SPAN = 2 * REACH + 1
BACK = 2 * REACH
EPS = 1e-05
FLOOR = -1e30
GROUPS = 2
STEP = 8
ATTEND = 16
AHEAD = 2
EARLY = 12
ORDER = (0, 8, 1, 7, 2, 6, 3, 5)

f32 = jnp.float32
bf16 = jnp.bfloat16


def normalize(values):
    mean = jnp.mean(values, axis=-1, keepdims=True)
    center = values - mean
    spread = jnp.mean(center * center, axis=-1, keepdims=True)
    return center * lax.rsqrt(spread + EPS)


def dot(a, b):
    return jnp.dot(a, b, preferred_element_type=f32)


def rows_to_lanes(tall, heads):
    rows = tall.shape[0] // heads
    return jnp.concatenate([tall[h * rows : (h + 1) * rows] for h in range(heads)], axis=1)


def other(slot):
    return slot - (slot > REACH)


def part(g, width):
    return slice(g * width, (g + 1) * width)


def kernel(
    n_dp,
    clip_h,
    media_h,
    table_h,
    latents_h,
    mgain_h,
    lgain_h,
    fgain_h,
    wq_h,
    wk_h,
    wv_h,
    wo_h,
    out_ref,
    clip_s,
    clip_v,
    near_clips,
    media,
    table,
    latents,
    mgain,
    lgain,
    fgain,
    wq,
    wkv,
    wo,
    stamps,
    norm_a,
    norm_b,
    scales,
    centered,
    kv0,
    p_a,
    p_b,
    p_c,
    p_d,
    kv1,
    accs,
    tops,
    totals,
    q_near_a,
    q_near_b,
    wide0,
    diagonal,
    part_acc,
    part_st,
    got_acc,
    got_st,
    attn_all,
    self_acc,
    self_st,
    state,
    local_sem,
    media_sem,
    clip_send,
    clip_recv,
    wo_send,
    wo_recv,
    acc_send,
    acc_recv,
    st_recv,
    q_recv,
    at_send,
    at_recv,
):
    frames, patches, width = media.shape
    inner = wq.shape[2]
    heads = inner // HEAD_DIM // GROUPS
    lat = latents.shape[0]
    hq = heads * lat
    hd = heads * HEAD_DIM
    me = lax.axis_index("dp")
    core = lax.axis_index("mp")

    def at(step):
        return (me + step, core)

    def near(step):
        return pl.when(me + step < n_dp if step > 0 else me + step >= 0)

    def beyond(step):
        return pl.when(me + step >= n_dp if step > 0 else me + step < 0)

    partner = (me, 1 - core)
    q_near = (q_near_a, q_near_b)

    barrier = pltpu.get_barrier_semaphore()
    for step in (*range(-BACK, 0), *range(1, REACH + 1)):

        @near(step)
        def _():
            pl.semaphore_signal(barrier, inc=1, device_id=at(step), device_id_type=MESH)

    pl.semaphore_signal(barrier, inc=1, device_id=partner, device_id_type=MESH)

    mine = pl.ds(pl.multiple_of(core * inner, inner), inner)
    step4 = 4

    def media_copy(i):
        rows = pl.ds(i * step4, step4)
        return pltpu.make_async_copy(media_h.at[rows], media.at[rows], media_sem.at[i])

    media_in = [media_copy(i) for i in range(frames // step4)]
    loads = [
        (clip_h, clip_v),
        (clip_h, clip_s),
        (table_h, table),
        (latents_h, latents),
        (lgain_h, lgain),
        (mgain_h, mgain),
        (fgain_h, fgain),
        (wq_h, wq),
    ]
    for g in range(GROUPS):
        columns = pl.ds(g * hd, hd)
        loads.append((wk_h.at[:, :, columns], wkv.at[:, :, pl.ds(2 * g * hd, hd)]))
        loads.append((wv_h.at[:, :, columns], wkv.at[:, :, pl.ds((2 * g + 1) * hd, hd)]))
    loads.append((wo_h, wo.at[:, mine, :]))
    loads = [pltpu.make_async_copy(a, b, local_sem.at[i]) for i, (a, b) in enumerate(loads)]
    for copy in loads[:2] + media_in + loads[2:]:
        copy.start()

    loads[0].wait()
    pl.semaphore_wait(barrier, jnp.minimum(BACK, n_dp - 1 - me) + jnp.minimum(REACH, me) + 1)
    clip_copies = [
        pltpu.make_async_remote_copy(
            src_ref=clip_v,
            dst_ref=near_clips.at[step - 1],
            send_sem=clip_send.at[step - 1],
            recv_sem=clip_recv.at[step - 1],
            device_id=at(step),
            device_id_type=MESH,
        )
        for step in range(1, BACK + 1)
    ]
    for step in range(BACK, 0, -1):
        near(step)(clip_copies[step - 1].start)
    wo_copy = pltpu.make_async_remote_copy(
        src_ref=wo_h,
        dst_ref=wo.at[:, mine, :],
        send_sem=wo_send,
        recv_sem=wo_recv,
        device_id=partner,
        device_id_type=MESH,
    )
    wo_copy.start()

    for step in range(1, BACK + 1):

        @beyond(-step)
        def _():
            near_clips[step - 1] = jnp.full(near_clips.shape[1:], -1, jnp.int32)

    for slot in ORDER:

        @beyond(REACH - slot)
        def _():
            for layer in range(LAYERS):
                for g in range(GROUPS):
                    got_st[layer, slot, 2 * g : 2 * g + 1, :] = jnp.full((1, hq), FLOOR, f32)
                    got_st[layer, slot, 2 * g + 1 : 2 * g + 2, :] = jnp.zeros((1, hq), f32)
                    got_acc[layer, g, slot] = jnp.zeros((HEAD_DIM, hq), bf16)

    chunk = 16

    def center(f, carry):
        for r in range(patches // chunk):
            x = media[f, part(r, chunk), :].astype(f32)
            centered[f, part(r, chunk), :] = x - jnp.mean(x, axis=-1, keepdims=True)
        return carry

    for i in range(frames // step4):
        media_in[i].wait()
        lax.fori_loop(i * step4, (i + 1) * step4, center, 0)

    row_head = lax.broadcasted_iota(jnp.int32, (hd, hq), 0) // HEAD_DIM
    lane_head = lax.broadcasted_iota(jnp.int32, (hd, hq), 1) // lat
    diagonal[...] = (row_head == lane_head).astype(f32).astype(bf16)
    piece_head = lax.broadcasted_iota(jnp.int32, (HEAD_DIM, hq), 1) // lat

    def widen(compact):
        return jnp.concatenate([compact] * heads, axis=0) * diagonal[...]

    def score(keys, wide):
        scores = dot(keys, wide)
        top = jnp.max(scores, axis=0, keepdims=True)
        expo = jnp.exp(scores - top)
        return top, jnp.sum(expo, axis=0, keepdims=True), expo.astype(bf16)

    def weigh(weights, values):
        full = lax.dot_general(values, weights, (((0,), (0,)), ((), ())), preferred_element_type=f32)
        acc = full[0:HEAD_DIM]
        for h in range(1, heads):
            acc = jnp.where(piece_head == h, full[part(h, HEAD_DIM)], acc)
        return acc

    def latent_side(layer):
        lat_norm = (normalize(state[...]) * lgain[layer : layer + 1, :]).astype(bf16)
        query = dot(lat_norm, wq[layer]) * (HEAD_DIM ** (-0.5))
        return lat_norm, [rows_to_lanes(query[:, part(g, hd)].T, heads).astype(bf16) for g in range(GROUPS)]

    def self_block(layer, lat_norm, compact):
        kv = dot(lat_norm, wkv[layer]).astype(bf16)
        for g in range(GROUPS):
            top, total, weights = score(kv[:, part(2 * g, hd)], widen(compact[g]))
            self_st[g, 0:1, :] = top
            self_st[g, 1:2, :] = total
            self_acc[g] = weigh(weights, kv[:, part(2 * g + 1, hd)])

    for copy in loads[1:-1]:
        copy.wait()
    state[...] = latents[...]
    lat_norm, compact = latent_side(0)
    self_block(0, lat_norm, compact)
    for g in range(GROUPS):
        wide0[g] = widen(compact[g])

    row = lax.broadcasted_iota(jnp.int32, (frames, frames), 0)
    lane = lax.broadcasted_iota(jnp.int32, (frames, frames), 1)
    clip_col = jnp.zeros((frames, 1), jnp.int32)
    frame_row = lax.broadcasted_iota(jnp.int32, (frames, 1), 0)
    for f in range(frames):
        clip_col = jnp.where(frame_row == f, clip_s[0, f], clip_col)
    slot_col = clip_col - me + REACH
    seen = jnp.where((clip_col == clip_v[...]) & (lane < row), 1.0, 0.0)
    for step in range(1, BACK + 1):
        near(-step)(clip_copies[step - 1].wait_recv)
    for step in range(1, BACK + 1):
        seen += jnp.where(clip_col == near_clips[step - 1], 1.0, 0.0)
    index = jnp.sum(seen, axis=1, keepdims=True).astype(jnp.int32)
    times = table.shape[0]
    picker = (lax.broadcasted_iota(jnp.int32, (frames, times), 1) == index).astype(f32).astype(bf16)
    stamp = dot(picker, table[...])
    stamps[...] = stamp - jnp.mean(stamp, axis=-1, keepdims=True)

    def norm_frame(f, dst):
        stamp = stamps[pl.ds(f, 1), :]
        for r in range(patches // chunk):
            rows = part(r, chunk)
            value = centered[f, rows, :] + stamp
            scale = lax.rsqrt(jnp.mean(value * value, axis=-1, keepdims=True) + EPS)
            scales[f, rows, :] = jnp.broadcast_to(scale, (chunk, 128))
            dst[rows, :] = (value * scale * mgain[0:1, :]).astype(bf16)

    def norm_frame1(f, dst):
        stamp = stamps[pl.ds(f, 1), :]
        for r in range(patches // chunk):
            rows = part(r, chunk)
            value = centered[f, rows, :] + stamp
            scale = jnp.concatenate([scales[f, rows, :]] * (width // 128), axis=1)
            dst[rows, :] = (value * scale * mgain[1:2, :]).astype(bf16)

    def project0(src, f):
        kv0[f] = dot(src[...], wkv[0]).astype(bf16)

    def project1(src, f):
        kv1[f] = dot(src[...], wkv[1]).astype(bf16)

    def score_frame(g, f, keys, wide, dst):
        tops[g, pl.ds(f, 1), :], totals[g, pl.ds(f, 1), :], dst[...] = score(keys, wide)

    p_all = (p_a, p_b, p_c, p_d)

    def norm_project(norm, project, start, stop, step):
        def several(i, carry):
            for j in range(step):
                f = step * i + j
                this, following = (norm_a, norm_b) if j % 2 == 0 else (norm_b, norm_a)
                norm(jnp.minimum(f + 1, frames - 1) if j == step - 1 else f + 1, following)
                project(this, f)
            return carry

        lax.fori_loop(start // step, stop // step, several, 0)

    norm_frame(0, norm_a)
    norm_project(norm_frame, project0, 0, frames, STEP)

    def attend(score_at, weigh_at):
        def several(i, carry):
            for j in range(ATTEND):
                f = ATTEND * i + j
                ahead = f + AHEAD
                score_at(jnp.minimum(ahead, frames - 1) if j + AHEAD >= ATTEND else ahead, p_all[(j + AHEAD) % len(p_all)])
                weigh_at(f, p_all[j % len(p_all)])
            return carry

        for j in range(AHEAD):
            score_at(j, p_all[j])
        lax.fori_loop(0, frames // ATTEND, several, 0)

    def score0(g, f, dst):
        score_frame(g, f, kv0[f, :, part(2 * g, hd)], wide0[g], dst)

    def weigh0(g, f, src):
        accs[g, f] = weigh(src[...], kv0[f, :, part(2 * g + 1, hd)])

    def gather_part(layer, g, slot):
        chosen = slot_col == slot
        top = jnp.max(jnp.where(chosen, tops[g], FLOOR), axis=0, keepdims=True)
        weight = jnp.where(chosen, jnp.exp(jnp.where(chosen, tops[g] - top, 0.0)), 0.0)
        acc = jnp.zeros((HEAD_DIM, hq), f32)
        for f in range(frames):
            acc += weight[f : f + 1, :] * accs[g, f]
        part_acc[layer, g, slot] = acc.astype(bf16)
        part_st[layer, slot, 2 * g : 2 * g + 1, :] = top
        part_st[layer, slot, 2 * g + 1 : 2 * g + 2, :] = jnp.sum(weight * totals[g], axis=0, keepdims=True)

    def part_copies(layer, g, slot):
        copies = [
            pltpu.make_async_remote_copy(
                src_ref=part_acc.at[layer, g, slot],
                dst_ref=got_acc.at[layer, g, slot],
                send_sem=acc_send.at[g, other(slot)],
                recv_sem=acc_recv.at[g, other(slot)],
                device_id=at(slot - REACH),
                device_id_type=MESH,
            )
        ]
        if g == GROUPS - 1:
            copies.append(
                pltpu.make_async_remote_copy(
                    src_ref=part_st.at[layer, slot],
                    dst_ref=got_st.at[layer, slot],
                    send_sem=clip_send.at[other(slot)],
                    recv_sem=st_recv.at[other(slot)],
                    device_id=at(slot - REACH),
                    device_id_type=MESH,
                )
            )
        return copies

    def send_parts(layer, g):
        for slot in ORDER:
            gather_part(layer, g, slot)
            copies = part_copies(layer, g, slot)

            @near(slot - REACH)
            def _():
                for copy in copies:
                    copy.start()

        gather_part(layer, g, REACH)

    def wait_parts(layer):
        for g in range(GROUPS):
            for slot in ORDER:
                copies = part_copies(layer, g, slot)

                @near(REACH - slot)
                def _():
                    for copy in copies:
                        copy.wait_recv()

    def wait_sent(layer):
        for slot in ORDER:

            @near(slot - REACH)
            def _():
                for g in range(GROUPS):
                    for copy in part_copies(layer, g, slot):
                        copy.wait_send()

    def merge_parts(layer, g):
        sources = [(self_st[g, 0:1, :], self_st[g, 1:2, :], self_acc.at[g])]
        for held_st, held_acc, slots in ((part_st, part_acc, (REACH,)), (got_st, got_acc, ORDER)):
            for slot in slots:
                held = (
                    held_st[layer, slot, 2 * g : 2 * g + 1, :],
                    held_st[layer, slot, 2 * g + 1 : 2 * g + 2, :],
                )
                sources.append((*held, held_acc.at[layer, g, slot]))
        best = functools.reduce(jnp.maximum, [top for top, _, _ in sources])
        whole = jnp.zeros_like(best)
        combined = jnp.zeros((HEAD_DIM, hq), f32)
        for top, total, acc in sources:
            weight = jnp.exp(top - best)
            whole += weight * total
            combined += weight * acc[...].astype(f32)
        return rows_to_lanes((combined / whole).T, heads).astype(bf16)

    def attn_copy(layer, g):
        columns = pl.ds(pl.multiple_of(core * inner + g * hd, hd), hd)
        return columns, pltpu.make_async_remote_copy(
            src_ref=attn_all.at[layer, :, columns],
            dst_ref=attn_all.at[layer, :, columns],
            send_sem=at_send.at[layer, g],
            recv_sem=at_recv.at[layer, g],
            device_id=partner,
            device_id_type=MESH,
        )

    def share_attn(layer, g):
        columns, copy = attn_copy(layer, g)
        attn_all[layer, :, columns] = merge_parts(layer, g)
        copy.start()

    def update_state(layer):
        theirs = pl.ds(pl.multiple_of((1 - core) * inner, inner), inner)
        state[...] += dot(attn_all[layer, :, mine], wo[layer, mine, :])
        for g in range(GROUPS):
            attn_copy(layer, g)[1].wait_recv()
        state[...] += dot(attn_all[layer, :, theirs], wo[layer, theirs, :])

    for step in range(1, BACK + 1):
        near(step)(clip_copies[step - 1].wait_send)
    for g in range(GROUPS):
        attend(functools.partial(score0, g), functools.partial(weigh0, g))
        send_parts(0, g)

    norm_frame1(0, norm_a)
    norm_project(norm_frame1, project1, 0, EARLY, 2)
    loads[-1].wait()
    wo_copy.wait()
    wait_parts(0)
    share_attn(0, 0)
    share_attn(0, 1)
    update_state(0)

    lat_norm, compact = latent_side(1)

    def q_copy(g, slot):
        return pltpu.make_async_remote_copy(
            src_ref=q_near[g].at[REACH],
            dst_ref=q_near[g].at[SPAN - 1 - slot],
            send_sem=acc_send.at[g, other(slot)],
            recv_sem=q_recv.at[g, other(SPAN - 1 - slot)],
            device_id=at(slot - REACH),
            device_id_type=MESH,
        )

    for g in range(GROUPS):
        q_near[g][REACH] = compact[g]
    wait_sent(0)
    for g in range(GROUPS):
        for slot in ORDER:
            near(slot - REACH)(q_copy(g, slot).start)
    self_block(1, lat_norm, compact)
    norm_project(norm_frame1, project1, EARLY, frames, 2)

    def score1(g, f, dst):
        slot = jnp.clip(clip_s[0, f] - me + REACH, 0, SPAN - 1)
        score_frame(g, f, kv1[f, :, part(2 * g, hd)], widen(q_near[g][slot]), dst)

    def weigh1(g, f, src):
        accs[g, f] = weigh(src[...], kv1[f, :, part(2 * g + 1, hd)])

    for g in range(GROUPS):
        for slot in ORDER:
            near(REACH - slot)(q_copy(g, slot).wait_recv)

        attend(functools.partial(score1, g), functools.partial(weigh1, g))
        for slot in ORDER:
            near(slot - REACH)(q_copy(g, slot).wait_send)
        send_parts(1, g)

    wait_parts(1)
    share_attn(1, 0)
    share_attn(1, 1)
    update_state(1)
    out_ref[...] = normalize(state[...]) * fgain[...]

    wait_sent(1)
    for layer in range(LAYERS):
        for g in range(GROUPS):
            attn_copy(layer, g)[1].wait_send()


def local(n_dp, media, slot_clip, table, latents, mgain, lgain, fgain, wq, wk, wv, wo):
    frames, patches, width = media.shape
    layers, _, inner = wq.shape
    heads = inner // HEAD_DIM // GROUPS
    lat = latents.shape[0]
    hq = heads * lat
    hd = heads * HEAD_DIM
    vmem, dma = pltpu.VMEM, pltpu.SemaphoreType.DMA
    scratch = [
        pltpu.SMEM((1, frames), jnp.int32),
        vmem((1, frames), jnp.int32),
        vmem((BACK, 1, frames), jnp.int32),
        vmem((frames, patches, width), bf16),
        vmem(table.shape, bf16),
        vmem(latents.shape, f32),
        vmem(mgain.shape, f32),
        vmem(lgain.shape, f32),
        vmem((1, width), f32),
        vmem(wq.shape, bf16),
        vmem((layers, width, 2 * inner), bf16),
        vmem((layers, 2 * inner, width), bf16),
        vmem((frames, width), f32),
        vmem((patches, width), bf16),
        vmem((patches, width), bf16),
        vmem((frames, patches, 128), f32),
        vmem((frames, patches, width), f32),
        vmem((frames, patches, 2 * inner), bf16),
        vmem((patches, hq), bf16),
        vmem((patches, hq), bf16),
        vmem((patches, hq), bf16),
        vmem((patches, hq), bf16),
        vmem((frames, patches, 2 * inner), bf16),
        vmem((GROUPS, frames, HEAD_DIM, hq), f32),
        vmem((GROUPS, frames, hq), f32),
        vmem((GROUPS, frames, hq), f32),
        vmem((SPAN, HEAD_DIM, hq), bf16),
        vmem((SPAN, HEAD_DIM, hq), bf16),
        vmem((GROUPS, hd, hq), bf16),
        vmem((hd, hq), bf16),
        vmem((layers, GROUPS, SPAN, HEAD_DIM, hq), bf16),
        vmem((layers, SPAN, 2 * GROUPS, hq), f32),
        vmem((layers, GROUPS, SPAN, HEAD_DIM, hq), bf16),
        vmem((layers, SPAN, 2 * GROUPS, hq), f32),
        vmem((layers, lat, 2 * inner), bf16),
        vmem((GROUPS, HEAD_DIM, hq), f32),
        vmem((GROUPS, 2, hq), f32),
        vmem(latents.shape, f32),
        dma((9 + 2 * GROUPS,)),
        dma((frames // 4,)),
        dma((BACK,)),
        dma((BACK,)),
        dma(()),
        dma(()),
        dma((GROUPS, BACK)),
        dma((GROUPS, BACK)),
        dma((BACK,)),
        dma((GROUPS, BACK)),
        dma((layers, GROUPS)),
        dma((layers, GROUPS)),
    ]
    result = pl.pallas_call(
        functools.partial(kernel, n_dp),
        out_shape=pltpu.VMEM(latents.shape, f32),
        in_specs=[pl.BlockSpec(memory_space=pltpu.HBM)] * 11,
        out_specs=pl.BlockSpec(memory_space=pltpu.VMEM),
        scratch_shapes=scratch,
        compiler_params=pltpu.CompilerParams(
            collective_id=0, has_side_effects=True, vmem_limit_bytes=56 * 1024 * 1024
        ),
        name="resample",
    )(slot_clip[None, :], media, table, latents, mgain, lgain, fgain[None, :], wq, wk, wv, wo)
    return result[None]


def solution(mesh):
    return jax.shard_map(
        functools.partial(local, mesh.shape["dp"]),
        mesh=mesh,
        in_specs=(
            P("dp", None, None),
            P("dp"),
            P(),
            P(),
            P(),
            P(),
            P(),
            P(None, None, "mp"),
            P(None, None, "mp"),
            P(None, None, "mp"),
            P(None, "mp", None),
        ),
        out_specs=P("dp", None, None),
        check_vma=False,
    )
```

```python
import functools

import jax
import jax.numpy as jnp
from jax import lax
from jax.experimental import pallas as pl
from jax.experimental.pallas import tpu as pltpu
from jax.sharding import PartitionSpec as P

MESH = pl.DeviceIdType.MESH
HEAD_DIM = 64
LAYERS = 2
REACH = 4
SPAN = 2 * REACH + 1
BACK = 2 * REACH
EPS = 1e-05
FLOOR = -1e30
GROUPS = 2
STEP = 8
ATTEND = 16
AHEAD = 2
EARLY = 12
ORDER = (0, 8, 1, 7, 2, 6, 3, 5)

f32 = jnp.float32
bf16 = jnp.bfloat16


def normalize(values):
    mean = jnp.mean(values, axis=-1, keepdims=True)
    center = values - mean
    spread = jnp.mean(center * center, axis=-1, keepdims=True)
    return center * lax.rsqrt(spread + EPS)


def dot(a, b):
    return jnp.dot(a, b, preferred_element_type=f32)


def rows_to_lanes(tall, heads):
    rows = tall.shape[0] // heads
    return jnp.concatenate([tall[h * rows : (h + 1) * rows] for h in range(heads)], axis=1)


def other(slot):
    return slot - (slot > REACH)


def part(g, width):
    return slice(g * width, (g + 1) * width)


def kernel(
    n_dp,
    clip_h,
    media_h,
    table_h,
    latents_h,
    mgain_h,
    lgain_h,
    fgain_h,
    wq_h,
    wk_h,
    wv_h,
    wo_h,
    out_ref,
    clip_s,
    clip_v,
    near_clips,
    media,
    table,
    latents,
    mgain,
    lgain,
    fgain,
    wq,
    wkv,
    wo,
    stamps,
    norm_a,
    norm_b,
    scales,
    centered,
    kv0,
    p_a,
    p_b,
    p_c,
    p_d,
    kv1,
    accs,
    tops,
    totals,
    q_near_a,
    q_near_b,
    wide0,
    diagonal,
    part_acc,
    part_st,
    got_acc,
    got_st,
    attn_all,
    self_acc,
    self_st,
    state,
    local_sem,
    media_sem,
    clip_send,
    clip_recv,
    wo_send,
    wo_recv,
    acc_send,
    acc_recv,
    st_recv,
    q_recv,
    at_send,
    at_recv,
):
    frames, patches, width = media.shape
    inner = wq.shape[2]
    heads = inner // HEAD_DIM // GROUPS
    lat = latents.shape[0]
    hq = heads * lat
    hd = heads * HEAD_DIM
    me = lax.axis_index("dp")
    core = lax.axis_index("mp")

    def at(step):
        return (me + step, core)

    def near(step):
        return pl.when(me + step < n_dp if step > 0 else me + step >= 0)

    def beyond(step):
        return pl.when(me + step >= n_dp if step > 0 else me + step < 0)

    partner = (me, 1 - core)
    q_near = (q_near_a, q_near_b)

    barrier = pltpu.get_barrier_semaphore()
    for step in (-4, 4, -5, -3, 3, -6, -2, 2, -7, -1, 1, -8):

        @near(step)
        def _():
            pl.semaphore_signal(barrier, inc=1, device_id=at(step), device_id_type=MESH)

    pl.semaphore_signal(barrier, inc=1, device_id=partner, device_id_type=MESH)

    mine = pl.ds(pl.multiple_of(core * inner, inner), inner)
    step4 = 4

    def media_copy(i):
        rows = pl.ds(i * step4, step4)
        return pltpu.make_async_copy(media_h.at[rows], media.at[rows], media_sem.at[i])

    media_in = [media_copy(i) for i in range(frames // step4)]
    loads = [
        (clip_h, clip_v),
        (clip_h, clip_s),
        (table_h, table),
        (latents_h, latents),
        (lgain_h, lgain),
        (mgain_h, mgain),
        (fgain_h, fgain),
        (wq_h, wq),
    ]
    for g in range(GROUPS):
        columns = pl.ds(g * hd, hd)
        loads.append((wk_h.at[:, :, columns], wkv.at[:, :, pl.ds(2 * g * hd, hd)]))
        loads.append((wv_h.at[:, :, columns], wkv.at[:, :, pl.ds((2 * g + 1) * hd, hd)]))
    loads.append((wo_h, wo.at[:, mine, :]))
    loads = [pltpu.make_async_copy(a, b, local_sem.at[i]) for i, (a, b) in enumerate(loads)]
    for copy in loads[:2] + media_in + loads[2:]:
        copy.start()

    loads[0].wait()
    pl.semaphore_wait(barrier, jnp.minimum(BACK, n_dp - 1 - me) + jnp.minimum(REACH, me) + 1)
    clip_copies = [
        pltpu.make_async_remote_copy(
            src_ref=clip_v,
            dst_ref=near_clips.at[step - 1],
            send_sem=clip_send.at[step - 1],
            recv_sem=clip_recv.at[step - 1],
            device_id=at(step),
            device_id_type=MESH,
        )
        for step in range(1, BACK + 1)
    ]
    for step in (4, 5, 3, 6, 2, 7, 1, 8):
        near(step)(clip_copies[step - 1].start)
    wo_copy = pltpu.make_async_remote_copy(
        src_ref=wo_h,
        dst_ref=wo.at[:, mine, :],
        send_sem=wo_send,
        recv_sem=wo_recv,
        device_id=partner,
        device_id_type=MESH,
    )
    wo_copy.start()

    for step in range(1, BACK + 1):

        @beyond(-step)
        def _():
            near_clips[step - 1] = jnp.full(near_clips.shape[1:], -1, jnp.int32)

    for slot in ORDER:

        @beyond(REACH - slot)
        def _():
            for layer in range(LAYERS):
                for g in range(GROUPS):
                    got_st[layer, slot, 2 * g : 2 * g + 1, :] = jnp.full((1, hq), FLOOR, f32)
                    got_st[layer, slot, 2 * g + 1 : 2 * g + 2, :] = jnp.zeros((1, hq), f32)
                    got_acc[layer, g, slot] = jnp.zeros((HEAD_DIM, hq), bf16)

    chunk = 16

    def center(f, carry):
        for r in range(patches // chunk):
            x = media[f, part(r, chunk), :].astype(f32)
            centered[f, part(r, chunk), :] = x - jnp.mean(x, axis=-1, keepdims=True)
        return carry

    for i in range(frames // step4):
        media_in[i].wait()
        lax.fori_loop(i * step4, (i + 1) * step4, center, 0)

    row_head = lax.broadcasted_iota(jnp.int32, (hd, hq), 0) // HEAD_DIM
    lane_head = lax.broadcasted_iota(jnp.int32, (hd, hq), 1) // lat
    diagonal[...] = (row_head == lane_head).astype(f32).astype(bf16)
    piece_head = lax.broadcasted_iota(jnp.int32, (HEAD_DIM, hq), 1) // lat

    def widen(compact):
        return jnp.concatenate([compact] * heads, axis=0) * diagonal[...]

    def score(keys, wide):
        scores = dot(keys, wide)
        top = jnp.max(scores, axis=0, keepdims=True)
        expo = jnp.exp(scores - top)
        return top, jnp.sum(expo, axis=0, keepdims=True), expo.astype(bf16)

    def weigh(weights, values):
        full = lax.dot_general(values, weights, (((0,), (0,)), ((), ())), preferred_element_type=f32)
        acc = full[0:HEAD_DIM]
        for h in range(1, heads):
            acc = jnp.where(piece_head == h, full[part(h, HEAD_DIM)], acc)
        return acc

    def latent_side(layer):
        lat_norm = (normalize(state[...]) * lgain[layer : layer + 1, :]).astype(bf16)
        query = dot(lat_norm, wq[layer]) * (HEAD_DIM ** (-0.5))
        return lat_norm, [rows_to_lanes(query[:, part(g, hd)].T, heads).astype(bf16) for g in range(GROUPS)]

    def self_block(layer, lat_norm, compact):
        kv = dot(lat_norm, wkv[layer]).astype(bf16)
        for g in range(GROUPS):
            top, total, weights = score(kv[:, part(2 * g, hd)], widen(compact[g]))
            self_st[g, 0:1, :] = top
            self_st[g, 1:2, :] = total
            self_acc[g] = weigh(weights, kv[:, part(2 * g + 1, hd)])

    for copy in loads[1:-1]:
        copy.wait()
    state[...] = latents[...]
    lat_norm, compact = latent_side(0)
    self_block(0, lat_norm, compact)
    for g in range(GROUPS):
        wide0[g] = widen(compact[g])

    row = lax.broadcasted_iota(jnp.int32, (frames, frames), 0)
    lane = lax.broadcasted_iota(jnp.int32, (frames, frames), 1)
    clip_col = jnp.zeros((frames, 1), jnp.int32)
    frame_row = lax.broadcasted_iota(jnp.int32, (frames, 1), 0)
    for f in range(frames):
        clip_col = jnp.where(frame_row == f, clip_s[0, f], clip_col)
    slot_col = clip_col - me + REACH
    seen = jnp.where((clip_col == clip_v[...]) & (lane < row), 1.0, 0.0)
    for step in range(1, BACK + 1):
        near(-step)(clip_copies[step - 1].wait_recv)
    for step in range(1, BACK + 1):
        seen += jnp.where(clip_col == near_clips[step - 1], 1.0, 0.0)
    index = jnp.sum(seen, axis=1, keepdims=True).astype(jnp.int32)
    times = table.shape[0]
    picker = (lax.broadcasted_iota(jnp.int32, (frames, times), 1) == index).astype(f32).astype(bf16)
    stamp = dot(picker, table[...])
    stamps[...] = stamp - jnp.mean(stamp, axis=-1, keepdims=True)

    def norm_frame(f, dst):
        stamp = stamps[pl.ds(f, 1), :]
        for r in range(patches // chunk):
            rows = part(r, chunk)
            value = centered[f, rows, :] + stamp
            scale = lax.rsqrt(jnp.mean(value * value, axis=-1, keepdims=True) + EPS)
            scales[f, rows, :] = jnp.broadcast_to(scale, (chunk, 128))
            dst[rows, :] = (value * scale * mgain[0:1, :]).astype(bf16)

    def norm_frame1(f, dst):
        stamp = stamps[pl.ds(f, 1), :]
        for r in range(patches // chunk):
            rows = part(r, chunk)
            value = centered[f, rows, :] + stamp
            scale = jnp.concatenate([scales[f, rows, :]] * (width // 128), axis=1)
            dst[rows, :] = (value * scale * mgain[1:2, :]).astype(bf16)

    def project0(src, f):
        kv0[f] = dot(src[...], wkv[0]).astype(bf16)

    def project1(src, f):
        kv1[f] = dot(src[...], wkv[1]).astype(bf16)

    def score_frame(g, f, keys, wide, dst):
        tops[g, pl.ds(f, 1), :], totals[g, pl.ds(f, 1), :], dst[...] = score(keys, wide)

    p_all = (p_a, p_b, p_c, p_d)

    def norm_project(norm, project, start, stop, step):
        def several(i, carry):
            for j in range(step):
                f = step * i + j
                this, following = (norm_a, norm_b) if j % 2 == 0 else (norm_b, norm_a)
                norm(jnp.minimum(f + 1, frames - 1) if j == step - 1 else f + 1, following)
                project(this, f)
            return carry

        lax.fori_loop(start // step, stop // step, several, 0)

    norm_frame(0, norm_a)
    norm_project(norm_frame, project0, 0, frames, STEP)

    def attend(score_at, weigh_at):
        def several(i, carry):
            for j in range(ATTEND):
                f = ATTEND * i + j
                ahead = f + AHEAD
                score_at(jnp.minimum(ahead, frames - 1) if j + AHEAD >= ATTEND else ahead, p_all[(j + AHEAD) % len(p_all)])
                weigh_at(f, p_all[j % len(p_all)])
            return carry

        for j in range(AHEAD):
            score_at(j, p_all[j])
        lax.fori_loop(0, frames // ATTEND, several, 0)

    def score0(g, f, dst):
        score_frame(g, f, kv0[f, :, part(2 * g, hd)], wide0[g], dst)

    def weigh0(g, f, src):
        accs[g, f] = weigh(src[...], kv0[f, :, part(2 * g + 1, hd)])

    def gather_part(layer, g, slot):
        chosen = slot_col == slot
        top = jnp.max(jnp.where(chosen, tops[g], FLOOR), axis=0, keepdims=True)
        weight = jnp.where(chosen, jnp.exp(jnp.where(chosen, tops[g] - top, 0.0)), 0.0)
        acc = jnp.zeros((HEAD_DIM, hq), f32)
        for f in range(frames):
            acc += weight[f : f + 1, :] * accs[g, f]
        part_acc[layer, g, slot] = acc.astype(bf16)
        part_st[layer, slot, 2 * g : 2 * g + 1, :] = top
        part_st[layer, slot, 2 * g + 1 : 2 * g + 2, :] = jnp.sum(weight * totals[g], axis=0, keepdims=True)

    def part_copies(layer, g, slot):
        copies = [
            pltpu.make_async_remote_copy(
                src_ref=part_acc.at[layer, g, slot],
                dst_ref=got_acc.at[layer, g, slot],
                send_sem=acc_send.at[g, other(slot)],
                recv_sem=acc_recv.at[g, other(slot)],
                device_id=at(slot - REACH),
                device_id_type=MESH,
            )
        ]
        if g == GROUPS - 1:
            copies.append(
                pltpu.make_async_remote_copy(
                    src_ref=part_st.at[layer, slot],
                    dst_ref=got_st.at[layer, slot],
                    send_sem=clip_send.at[other(slot)],
                    recv_sem=st_recv.at[other(slot)],
                    device_id=at(slot - REACH),
                    device_id_type=MESH,
                )
            )
        return copies

    def send_parts(layer, g):
        for slot in ORDER:
            gather_part(layer, g, slot)
            copies = part_copies(layer, g, slot)

            @near(slot - REACH)
            def _():
                for copy in copies:
                    copy.start()

        gather_part(layer, g, REACH)

    def wait_parts(layer):
        for g in range(GROUPS):
            for slot in ORDER:
                copies = part_copies(layer, g, slot)

                @near(REACH - slot)
                def _():
                    for copy in copies:
                        copy.wait_recv()

    def wait_sent(layer):
        for slot in ORDER:

            @near(slot - REACH)
            def _():
                for g in range(GROUPS):
                    for copy in part_copies(layer, g, slot):
                        copy.wait_send()

    def merge_parts(layer, g):
        sources = [(self_st[g, 0:1, :], self_st[g, 1:2, :], self_acc.at[g])]
        for held_st, held_acc, slots in ((part_st, part_acc, (REACH,)), (got_st, got_acc, ORDER)):
            for slot in slots:
                held = (
                    held_st[layer, slot, 2 * g : 2 * g + 1, :],
                    held_st[layer, slot, 2 * g + 1 : 2 * g + 2, :],
                )
                sources.append((*held, held_acc.at[layer, g, slot]))
        best = functools.reduce(jnp.maximum, [top for top, _, _ in sources])
        whole = jnp.zeros_like(best)
        combined = jnp.zeros((HEAD_DIM, hq), f32)
        for top, total, acc in sources:
            weight = jnp.exp(top - best)
            whole += weight * total
            combined += weight * acc[...].astype(f32)
        return rows_to_lanes((combined / whole).T, heads).astype(bf16)

    def attn_copy(layer):
        return pltpu.make_async_remote_copy(
            src_ref=attn_all.at[layer, :, mine],
            dst_ref=attn_all.at[layer, :, mine],
            send_sem=at_send.at[layer],
            recv_sem=at_recv.at[layer],
            device_id=partner,
            device_id_type=MESH,
        )

    def share_attn(layer):
        attn_all[layer, :, mine] = jnp.concatenate([merge_parts(layer, g) for g in range(GROUPS)], axis=1)
        attn_copy(layer).start()

    def update_state(layer):
        theirs = pl.ds(pl.multiple_of((1 - core) * inner, inner), inner)
        state[...] += dot(attn_all[layer, :, mine], wo[layer, mine, :])
        attn_copy(layer).wait_recv()
        state[...] += dot(attn_all[layer, :, theirs], wo[layer, theirs, :])

    for step in range(1, BACK + 1):
        near(step)(clip_copies[step - 1].wait_send)
    for g in range(GROUPS):
        attend(functools.partial(score0, g), functools.partial(weigh0, g))
        send_parts(0, g)

    norm_frame1(0, norm_a)
    norm_project(norm_frame1, project1, 0, EARLY, 2)
    loads[-1].wait()
    wo_copy.wait()
    wait_sent(0)
    wait_parts(0)
    share_attn(0)
    update_state(0)

    lat_norm, compact = latent_side(1)

    def q_copy(g, slot):
        return pltpu.make_async_remote_copy(
            src_ref=q_near[g].at[REACH],
            dst_ref=q_near[g].at[SPAN - 1 - slot],
            send_sem=acc_send.at[g, other(slot)],
            recv_sem=q_recv.at[g, other(SPAN - 1 - slot)],
            device_id=at(slot - REACH),
            device_id_type=MESH,
        )

    for g in range(GROUPS):
        q_near[g][REACH] = compact[g]
    for g in range(GROUPS):
        for slot in ORDER:
            near(slot - REACH)(q_copy(g, slot).start)
    self_block(1, lat_norm, compact)
    norm_project(norm_frame1, project1, EARLY, frames, 2)

    def score1(g, f, dst):
        slot = jnp.clip(clip_s[0, f] - me + REACH, 0, SPAN - 1)
        score_frame(g, f, kv1[f, :, part(2 * g, hd)], widen(q_near[g][slot]), dst)

    def weigh1(g, f, src):
        accs[g, f] = weigh(src[...], kv1[f, :, part(2 * g + 1, hd)])

    for g in range(GROUPS):
        for slot in ORDER:
            near(slot - REACH)(q_copy(g, slot).wait_send)
        for slot in ORDER:
            near(REACH - slot)(q_copy(g, slot).wait_recv)

        attend(functools.partial(score1, g), functools.partial(weigh1, g))
        send_parts(1, g)

    wait_parts(1)
    share_attn(1)
    update_state(1)
    out_ref[...] = normalize(state[...]) * fgain[...]

    wait_sent(1)
    for layer in range(LAYERS):
        attn_copy(layer).wait_send()


def local(n_dp, media, slot_clip, table, latents, mgain, lgain, fgain, wq, wk, wv, wo):
    frames, patches, width = media.shape
    layers, _, inner = wq.shape
    heads = inner // HEAD_DIM // GROUPS
    lat = latents.shape[0]
    hq = heads * lat
    hd = heads * HEAD_DIM
    vmem, dma = pltpu.VMEM, pltpu.SemaphoreType.DMA
    scratch = [
        pltpu.SMEM((1, frames), jnp.int32),
        vmem((1, frames), jnp.int32),
        vmem((BACK, 1, frames), jnp.int32),
        vmem((frames, patches, width), bf16),
        vmem(table.shape, bf16),
        vmem(latents.shape, f32),
        vmem(mgain.shape, f32),
        vmem(lgain.shape, f32),
        vmem((1, width), f32),
        vmem(wq.shape, bf16),
        vmem((layers, width, 2 * inner), bf16),
        vmem((layers, 2 * inner, width), bf16),
        vmem((frames, width), f32),
        vmem((patches, width), bf16),
        vmem((patches, width), bf16),
        vmem((frames, patches, 128), f32),
        vmem((frames, patches, width), f32),
        vmem((frames, patches, 2 * inner), bf16),
        vmem((patches, hq), bf16),
        vmem((patches, hq), bf16),
        vmem((patches, hq), bf16),
        vmem((patches, hq), bf16),
        vmem((frames, patches, 2 * inner), bf16),
        vmem((GROUPS, frames, HEAD_DIM, hq), f32),
        vmem((GROUPS, frames, hq), f32),
        vmem((GROUPS, frames, hq), f32),
        vmem((SPAN, HEAD_DIM, hq), bf16),
        vmem((SPAN, HEAD_DIM, hq), bf16),
        vmem((GROUPS, hd, hq), bf16),
        vmem((hd, hq), bf16),
        vmem((layers, GROUPS, SPAN, HEAD_DIM, hq), bf16),
        vmem((layers, SPAN, 2 * GROUPS, hq), f32),
        vmem((layers, GROUPS, SPAN, HEAD_DIM, hq), bf16),
        vmem((layers, SPAN, 2 * GROUPS, hq), f32),
        vmem((layers, lat, 2 * inner), bf16),
        vmem((GROUPS, HEAD_DIM, hq), f32),
        vmem((GROUPS, 2, hq), f32),
        vmem(latents.shape, f32),
        dma((9 + 2 * GROUPS,)),
        dma((frames // 4,)),
        dma((BACK,)),
        dma((BACK,)),
        dma(()),
        dma(()),
        dma((GROUPS, BACK)),
        dma((GROUPS, BACK)),
        dma((BACK,)),
        dma((GROUPS, BACK)),
        dma((layers,)),
        dma((layers,)),
    ]
    result = pl.pallas_call(
        functools.partial(kernel, n_dp),
        out_shape=pltpu.VMEM(latents.shape, f32),
        in_specs=[pl.BlockSpec(memory_space=pltpu.HBM)] * 11,
        out_specs=pl.BlockSpec(memory_space=pltpu.VMEM),
        scratch_shapes=scratch,
        compiler_params=pltpu.CompilerParams(
            collective_id=0, has_side_effects=True, vmem_limit_bytes=56 * 1024 * 1024
        ),
        name="resample",
    )(slot_clip[None, :], media, table, latents, mgain, lgain, fgain[None, :], wq, wk, wv, wo)
    return result[None]


def solution(mesh):
    return jax.shard_map(
        functools.partial(local, mesh.shape["dp"]),
        mesh=mesh,
        in_specs=(
            P("dp", None, None),
            P("dp"),
            P(),
            P(),
            P(),
            P(),
            P(),
            P(None, None, "mp"),
            P(None, None, "mp"),
            P(None, None, "mp"),
            P(None, "mp", None),
        ),
        out_specs=P("dp", None, None),
        check_vma=False,
    )
```

```python
import functools

import jax
import jax.numpy as jnp
from jax import lax
from jax.experimental import pallas as pl
from jax.experimental.pallas import tpu as pltpu
from jax.sharding import PartitionSpec as P

MESH = pl.DeviceIdType.MESH
HEAD_DIM = 64
LAYERS = 2
REACH = 4
SPAN = 2 * REACH + 1
BACK = 2 * REACH
EPS = 1e-05
FLOOR = -1e30
GROUPS = 2
STEP = 8
ATTEND = 16
AHEAD = 2
EARLY = 12
ORDER = (0, 8, 1, 7, 2, 6, 3, 5)

f32 = jnp.float32
bf16 = jnp.bfloat16


def normalize(values):
    mean = jnp.mean(values, axis=-1, keepdims=True)
    center = values - mean
    spread = jnp.mean(center * center, axis=-1, keepdims=True)
    return center * lax.rsqrt(spread + EPS)


def dot(a, b):
    return jnp.dot(a, b, preferred_element_type=f32)


def rows_to_lanes(tall, heads):
    rows = tall.shape[0] // heads
    return jnp.concatenate([tall[h * rows : (h + 1) * rows] for h in range(heads)], axis=1)


def other(slot):
    return slot - (slot > REACH)


def part(g, width):
    return slice(g * width, (g + 1) * width)


def kernel(
    n_dp,
    clip_h,
    media_h,
    table_h,
    latents_h,
    mgain_h,
    lgain_h,
    fgain_h,
    wq_h,
    wk_h,
    wv_h,
    wo_h,
    out_ref,
    clip_s,
    clip_v,
    near_clips,
    media,
    table,
    latents,
    mgain,
    lgain,
    fgain,
    wq,
    wkv,
    wo,
    stamps,
    norm_a,
    norm_b,
    scales,
    centered,
    kv0,
    p_a,
    p_b,
    p_c,
    p_d,
    kv1,
    accs,
    tops,
    totals,
    q_near_a,
    q_near_b,
    wide0,
    diagonal,
    part_acc,
    part_st,
    got_acc,
    got_st,
    attn_all,
    self_acc,
    self_st,
    state,
    local_sem,
    media_sem,
    clip_send,
    clip_recv,
    wo_send,
    wo_recv,
    acc_send,
    acc_recv,
    st_recv,
    q_recv,
    at_send,
    at_recv,
):
    frames, patches, width = media.shape
    inner = wq.shape[2]
    heads = inner // HEAD_DIM // GROUPS
    lat = latents.shape[0]
    hq = heads * lat
    hd = heads * HEAD_DIM
    me = lax.axis_index("dp")
    core = lax.axis_index("mp")

    def at(step):
        return (me + step, core)

    def near(step):
        return pl.when(me + step < n_dp if step > 0 else me + step >= 0)

    def beyond(step):
        return pl.when(me + step >= n_dp if step > 0 else me + step < 0)

    partner = (me, 1 - core)
    q_near = (q_near_a, q_near_b)

    barrier = pltpu.get_barrier_semaphore()
    for step in (-4, 4, -5, -3, 3, -6, -2, 2, -7, -1, 1, -8):

        @near(step)
        def _():
            pl.semaphore_signal(barrier, inc=1, device_id=at(step), device_id_type=MESH)

    pl.semaphore_signal(barrier, inc=1, device_id=partner, device_id_type=MESH)

    mine = pl.ds(pl.multiple_of(core * inner, inner), inner)
    step4 = 4

    def media_copy(i):
        rows = pl.ds(i * step4, step4)
        return pltpu.make_async_copy(media_h.at[rows], media.at[rows], media_sem.at[i])

    media_in = [media_copy(i) for i in range(frames // step4)]
    loads = [
        (clip_h, clip_v),
        (clip_h, clip_s),
        (table_h, table),
        (latents_h, latents),
        (lgain_h, lgain),
        (mgain_h, mgain),
        (fgain_h, fgain),
        (wq_h, wq),
    ]
    for g in range(GROUPS):
        columns = pl.ds(g * hd, hd)
        loads.append((wk_h.at[:, :, columns], wkv.at[:, :, pl.ds(2 * g * hd, hd)]))
        loads.append((wv_h.at[:, :, columns], wkv.at[:, :, pl.ds((2 * g + 1) * hd, hd)]))
    loads.append((wo_h, wo.at[:, mine, :]))
    loads = [pltpu.make_async_copy(a, b, local_sem.at[i]) for i, (a, b) in enumerate(loads)]
    for copy in loads[:2] + media_in + loads[2:]:
        copy.start()

    loads[0].wait()
    pl.semaphore_wait(barrier, jnp.minimum(BACK, n_dp - 1 - me) + jnp.minimum(REACH, me) + 1)
    clip_copies = [
        pltpu.make_async_remote_copy(
            src_ref=clip_v,
            dst_ref=near_clips.at[step - 1],
            send_sem=clip_send.at[step - 1],
            recv_sem=clip_recv.at[step - 1],
            device_id=at(step),
            device_id_type=MESH,
        )
        for step in range(1, BACK + 1)
    ]
    for step in (4, 5, 3, 6, 2, 7, 1, 8):
        near(step)(clip_copies[step - 1].start)
    wo_copy = pltpu.make_async_remote_copy(
        src_ref=wo_h,
        dst_ref=wo.at[:, mine, :],
        send_sem=wo_send,
        recv_sem=wo_recv,
        device_id=partner,
        device_id_type=MESH,
    )
    wo_copy.start()

    for step in range(1, BACK + 1):

        @beyond(-step)
        def _():
            near_clips[step - 1] = jnp.full(near_clips.shape[1:], -1, jnp.int32)

    for slot in ORDER:

        @beyond(REACH - slot)
        def _():
            for layer in range(LAYERS):
                for g in range(GROUPS):
                    got_st[layer, slot, 2 * g : 2 * g + 1, :] = jnp.full((1, hq), FLOOR, f32)
                    got_st[layer, slot, 2 * g + 1 : 2 * g + 2, :] = jnp.zeros((1, hq), f32)
                    got_acc[layer, g, slot] = jnp.zeros((HEAD_DIM, hq), bf16)

    chunk = 16

    def center(f, carry):
        for r in range(patches // chunk):
            x = media[f, part(r, chunk), :].astype(f32)
            centered[f, part(r, chunk), :] = x - jnp.mean(x, axis=-1, keepdims=True)
        return carry

    for i in range(frames // step4):
        media_in[i].wait()
        lax.fori_loop(i * step4, (i + 1) * step4, center, 0)

    row_head = lax.broadcasted_iota(jnp.int32, (hd, hq), 0) // HEAD_DIM
    lane_head = lax.broadcasted_iota(jnp.int32, (hd, hq), 1) // lat
    diagonal[...] = (row_head == lane_head).astype(f32).astype(bf16)
    piece_head = lax.broadcasted_iota(jnp.int32, (HEAD_DIM, hq), 1) // lat

    def widen(compact):
        return jnp.concatenate([compact] * heads, axis=0) * diagonal[...]

    def score(keys, wide):
        scores = dot(keys, wide)
        top = jnp.max(scores, axis=0, keepdims=True)
        expo = jnp.exp(scores - top)
        return top, jnp.sum(expo, axis=0, keepdims=True), expo.astype(bf16)

    def weigh(weights, values):
        full = lax.dot_general(values, weights, (((0,), (0,)), ((), ())), preferred_element_type=f32)
        acc = full[0:HEAD_DIM]
        for h in range(1, heads):
            acc = jnp.where(piece_head == h, full[part(h, HEAD_DIM)], acc)
        return acc

    def latent_side(layer):
        lat_norm = (normalize(state[...]) * lgain[layer : layer + 1, :]).astype(bf16)
        query = dot(lat_norm, wq[layer]) * (HEAD_DIM ** (-0.5))
        return lat_norm, [rows_to_lanes(query[:, part(g, hd)].T, heads).astype(bf16) for g in range(GROUPS)]

    def self_block(layer, lat_norm, compact):
        kv = dot(lat_norm, wkv[layer]).astype(bf16)
        for g in range(GROUPS):
            top, total, weights = score(kv[:, part(2 * g, hd)], widen(compact[g]))
            self_st[g, 0:1, :] = top
            self_st[g, 1:2, :] = total
            self_acc[g] = weigh(weights, kv[:, part(2 * g + 1, hd)])

    for copy in loads[1:-1]:
        copy.wait()
    state[...] = latents[...]
    lat_norm, compact = latent_side(0)
    self_block(0, lat_norm, compact)
    for g in range(GROUPS):
        wide0[g] = widen(compact[g])

    row = lax.broadcasted_iota(jnp.int32, (frames, frames), 0)
    lane = lax.broadcasted_iota(jnp.int32, (frames, frames), 1)
    clip_col = jnp.zeros((frames, 1), jnp.int32)
    frame_row = lax.broadcasted_iota(jnp.int32, (frames, 1), 0)
    for f in range(frames):
        clip_col = jnp.where(frame_row == f, clip_s[0, f], clip_col)
    slot_col = clip_col - me + REACH
    seen = jnp.where((clip_col == clip_v[...]) & (lane < row), 1.0, 0.0)
    for step in range(1, BACK + 1):
        near(-step)(clip_copies[step - 1].wait_recv)
    for step in range(1, BACK + 1):
        seen += jnp.where(clip_col == near_clips[step - 1], 1.0, 0.0)
    index = jnp.sum(seen, axis=1, keepdims=True).astype(jnp.int32)
    times = table.shape[0]
    picker = (lax.broadcasted_iota(jnp.int32, (frames, times), 1) == index).astype(f32).astype(bf16)
    stamp = dot(picker, table[...])
    stamps[...] = stamp - jnp.mean(stamp, axis=-1, keepdims=True)

    def norm_frame(f, dst):
        stamp = stamps[pl.ds(f, 1), :]
        for r in range(patches // chunk):
            rows = part(r, chunk)
            value = centered[f, rows, :] + stamp
            scale = lax.rsqrt(jnp.mean(value * value, axis=-1, keepdims=True) + EPS)
            scales[f, rows, :] = jnp.broadcast_to(scale, (chunk, 128))
            dst[rows, :] = (value * scale * mgain[0:1, :]).astype(bf16)

    def norm_frame1(f, dst):
        stamp = stamps[pl.ds(f, 1), :]
        for r in range(patches // chunk):
            rows = part(r, chunk)
            value = centered[f, rows, :] + stamp
            scale = jnp.concatenate([scales[f, rows, :]] * (width // 128), axis=1)
            dst[rows, :] = (value * scale * mgain[1:2, :]).astype(bf16)

    def project0(src, f):
        kv0[f] = dot(src[...], wkv[0]).astype(bf16)

    def project1(src, f):
        kv1[f] = dot(src[...], wkv[1]).astype(bf16)

    def score_frame(g, f, keys, wide, dst):
        tops[g, pl.ds(f, 1), :], totals[g, pl.ds(f, 1), :], dst[...] = score(keys, wide)

    p_all = (p_a, p_b, p_c, p_d)

    def norm_project(norm, project, start, stop, step):
        def several(i, carry):
            for j in range(step):
                f = step * i + j
                this, following = (norm_a, norm_b) if j % 2 == 0 else (norm_b, norm_a)
                norm(jnp.minimum(f + 1, frames - 1) if j == step - 1 else f + 1, following)
                project(this, f)
            return carry

        lax.fori_loop(start // step, stop // step, several, 0)

    norm_frame(0, norm_a)
    norm_project(norm_frame, project0, 0, frames, STEP)

    def attend(score_at, weigh_at):
        def several(i, carry):
            for j in range(ATTEND):
                f = ATTEND * i + j
                ahead = f + AHEAD
                score_at(jnp.minimum(ahead, frames - 1) if j + AHEAD >= ATTEND else ahead, p_all[(j + AHEAD) % len(p_all)])
                weigh_at(f, p_all[j % len(p_all)])
            return carry

        for j in range(AHEAD):
            score_at(j, p_all[j])
        lax.fori_loop(0, frames // ATTEND, several, 0)

    def score0(g, f, dst):
        score_frame(g, f, kv0[f, :, part(2 * g, hd)], wide0[g], dst)

    def weigh0(g, f, src):
        accs[g, f] = weigh(src[...], kv0[f, :, part(2 * g + 1, hd)])

    def gather_part(layer, g, slot):
        chosen = slot_col == slot
        top = jnp.max(jnp.where(chosen, tops[g], FLOOR), axis=0, keepdims=True)
        weight = jnp.where(chosen, jnp.exp(jnp.where(chosen, tops[g] - top, 0.0)), 0.0)
        acc = jnp.zeros((HEAD_DIM, hq), f32)
        for f in range(frames):
            acc += weight[f : f + 1, :] * accs[g, f]
        part_acc[layer, g, slot] = acc.astype(bf16)
        part_st[layer, slot, 2 * g : 2 * g + 1, :] = top
        part_st[layer, slot, 2 * g + 1 : 2 * g + 2, :] = jnp.sum(weight * totals[g], axis=0, keepdims=True)

    def part_copies(layer, g, slot):
        copies = [
            pltpu.make_async_remote_copy(
                src_ref=part_acc.at[layer, g, slot],
                dst_ref=got_acc.at[layer, g, slot],
                send_sem=acc_send.at[g, other(slot)],
                recv_sem=acc_recv.at[g, other(slot)],
                device_id=at(slot - REACH),
                device_id_type=MESH,
            )
        ]
        if g == GROUPS - 1:
            copies.append(
                pltpu.make_async_remote_copy(
                    src_ref=part_st.at[layer, slot],
                    dst_ref=got_st.at[layer, slot],
                    send_sem=clip_send.at[other(slot)],
                    recv_sem=st_recv.at[other(slot)],
                    device_id=at(slot - REACH),
                    device_id_type=MESH,
                )
            )
        return copies

    def send_parts(layer, g):
        for first in range(0, len(ORDER), 2):
            for slot in ORDER[first : first + 2]:
                gather_part(layer, g, slot)
            for slot in ORDER[first : first + 2]:
                copies = part_copies(layer, g, slot)

                @near(slot - REACH)
                def _():
                    for copy in copies:
                        copy.start()


    def wait_parts(layer):
        for g in range(GROUPS):
            gather_part(layer, g, REACH)
        for g in range(GROUPS):
            for slot in ORDER:
                copies = part_copies(layer, g, slot)

                @near(REACH - slot)
                def _():
                    for copy in copies:
                        copy.wait_recv()

    def wait_sent(layer):
        for slot in ORDER:

            @near(slot - REACH)
            def _():
                for g in range(GROUPS):
                    for copy in part_copies(layer, g, slot):
                        copy.wait_send()

    def merge_parts(layer, g):
        sources = [(self_st[g, 0:1, :], self_st[g, 1:2, :], self_acc.at[g])]
        for held_st, held_acc, slots in ((part_st, part_acc, (REACH,)), (got_st, got_acc, ORDER)):
            for slot in slots:
                held = (
                    held_st[layer, slot, 2 * g : 2 * g + 1, :],
                    held_st[layer, slot, 2 * g + 1 : 2 * g + 2, :],
                )
                sources.append((*held, held_acc.at[layer, g, slot]))
        best = functools.reduce(jnp.maximum, [top for top, _, _ in sources])
        whole = jnp.zeros_like(best)
        combined = jnp.zeros((HEAD_DIM, hq), f32)
        for top, total, acc in sources:
            weight = jnp.exp(top - best)
            whole += weight * total
            combined += weight * acc[...].astype(f32)
        return rows_to_lanes((combined / whole).T, heads).astype(bf16)

    def attn_copy(layer):
        return pltpu.make_async_remote_copy(
            src_ref=attn_all.at[layer, :, mine],
            dst_ref=attn_all.at[layer, :, mine],
            send_sem=at_send.at[layer],
            recv_sem=at_recv.at[layer],
            device_id=partner,
            device_id_type=MESH,
        )

    def share_attn(layer):
        attn_all[layer, :, mine] = jnp.concatenate([merge_parts(layer, g) for g in range(GROUPS)], axis=1)
        attn_copy(layer).start()

    def update_state(layer):
        theirs = pl.ds(pl.multiple_of((1 - core) * inner, inner), inner)
        state[...] += dot(attn_all[layer, :, mine], wo[layer, mine, :])
        attn_copy(layer).wait_recv()
        state[...] += dot(attn_all[layer, :, theirs], wo[layer, theirs, :])

    for step in range(1, BACK + 1):
        near(step)(clip_copies[step - 1].wait_send)
    for g in range(GROUPS):
        attend(functools.partial(score0, g), functools.partial(weigh0, g))
        send_parts(0, g)

    norm_frame1(0, norm_a)
    norm_project(norm_frame1, project1, 0, EARLY, 2)
    loads[-1].wait()
    wo_copy.wait()
    wait_sent(0)
    wait_parts(0)
    share_attn(0)
    update_state(0)

    lat_norm, compact = latent_side(1)

    def q_copy(g, slot):
        return pltpu.make_async_remote_copy(
            src_ref=q_near[g].at[REACH],
            dst_ref=q_near[g].at[SPAN - 1 - slot],
            send_sem=acc_send.at[g, other(slot)],
            recv_sem=q_recv.at[g, other(SPAN - 1 - slot)],
            device_id=at(slot - REACH),
            device_id_type=MESH,
        )

    for g in range(GROUPS):
        q_near[g][REACH] = compact[g]
    for g in range(GROUPS):
        for slot in ORDER:
            near(slot - REACH)(q_copy(g, slot).start)
    self_block(1, lat_norm, compact)
    norm_project(norm_frame1, project1, EARLY, frames, 2)

    def score1(g, f, dst):
        slot = jnp.clip(clip_s[0, f] - me + REACH, 0, SPAN - 1)
        score_frame(g, f, kv1[f, :, part(2 * g, hd)], widen(q_near[g][slot]), dst)

    def weigh1(g, f, src):
        accs[g, f] = weigh(src[...], kv1[f, :, part(2 * g + 1, hd)])

    for g in range(GROUPS):
        for slot in ORDER:
            near(slot - REACH)(q_copy(g, slot).wait_send)
        for slot in ORDER:
            near(REACH - slot)(q_copy(g, slot).wait_recv)

        attend(functools.partial(score1, g), functools.partial(weigh1, g))
        send_parts(1, g)

    wait_parts(1)
    share_attn(1)
    update_state(1)
    out_ref[...] = normalize(state[...]) * fgain[...]

    wait_sent(1)
    for layer in range(LAYERS):
        attn_copy(layer).wait_send()


def local(n_dp, media, slot_clip, table, latents, mgain, lgain, fgain, wq, wk, wv, wo):
    frames, patches, width = media.shape
    layers, _, inner = wq.shape
    heads = inner // HEAD_DIM // GROUPS
    lat = latents.shape[0]
    hq = heads * lat
    hd = heads * HEAD_DIM
    vmem, dma = pltpu.VMEM, pltpu.SemaphoreType.DMA
    scratch = [
        pltpu.SMEM((1, frames), jnp.int32),
        vmem((1, frames), jnp.int32),
        vmem((BACK, 1, frames), jnp.int32),
        vmem((frames, patches, width), bf16),
        vmem(table.shape, bf16),
        vmem(latents.shape, f32),
        vmem(mgain.shape, f32),
        vmem(lgain.shape, f32),
        vmem((1, width), f32),
        vmem(wq.shape, bf16),
        vmem((layers, width, 2 * inner), bf16),
        vmem((layers, 2 * inner, width), bf16),
        vmem((frames, width), f32),
        vmem((patches, width), bf16),
        vmem((patches, width), bf16),
        vmem((frames, patches, 128), f32),
        vmem((frames, patches, width), f32),
        vmem((frames, patches, 2 * inner), bf16),
        vmem((patches, hq), bf16),
        vmem((patches, hq), bf16),
        vmem((patches, hq), bf16),
        vmem((patches, hq), bf16),
        vmem((frames, patches, 2 * inner), bf16),
        vmem((GROUPS, frames, HEAD_DIM, hq), f32),
        vmem((GROUPS, frames, hq), f32),
        vmem((GROUPS, frames, hq), f32),
        vmem((SPAN, HEAD_DIM, hq), bf16),
        vmem((SPAN, HEAD_DIM, hq), bf16),
        vmem((GROUPS, hd, hq), bf16),
        vmem((hd, hq), bf16),
        vmem((layers, GROUPS, SPAN, HEAD_DIM, hq), bf16),
        vmem((layers, SPAN, 2 * GROUPS, hq), f32),
        vmem((layers, GROUPS, SPAN, HEAD_DIM, hq), bf16),
        vmem((layers, SPAN, 2 * GROUPS, hq), f32),
        vmem((layers, lat, 2 * inner), bf16),
        vmem((GROUPS, HEAD_DIM, hq), f32),
        vmem((GROUPS, 2, hq), f32),
        vmem(latents.shape, f32),
        dma((9 + 2 * GROUPS,)),
        dma((frames // 4,)),
        dma((BACK,)),
        dma((BACK,)),
        dma(()),
        dma(()),
        dma((GROUPS, BACK)),
        dma((GROUPS, BACK)),
        dma((BACK,)),
        dma((GROUPS, BACK)),
        dma((layers,)),
        dma((layers,)),
    ]
    result = pl.pallas_call(
        functools.partial(kernel, n_dp),
        out_shape=pltpu.VMEM(latents.shape, f32),
        in_specs=[pl.BlockSpec(memory_space=pltpu.HBM)] * 11,
        out_specs=pl.BlockSpec(memory_space=pltpu.VMEM),
        scratch_shapes=scratch,
        compiler_params=pltpu.CompilerParams(
            collective_id=0, has_side_effects=True, vmem_limit_bytes=56 * 1024 * 1024
        ),
        name="resample",
    )(slot_clip[None, :], media, table, latents, mgain, lgain, fgain[None, :], wq, wk, wv, wo)
    return result[None]


def solution(mesh):
    return jax.shard_map(
        functools.partial(local, mesh.shape["dp"]),
        mesh=mesh,
        in_specs=(
            P("dp", None, None),
            P("dp"),
            P(),
            P(),
            P(),
            P(),
            P(),
            P(None, None, "mp"),
            P(None, None, "mp"),
            P(None, None, "mp"),
            P(None, "mp", None),
        ),
        out_specs=P("dp", None, None),
        check_vma=False,
    )
```
